1024 devices in a mesh: gx: 4 (over x), gy: 16 (over y, z_hi), gz: 16 (over z_lo, core).
Axes of the slice: x: 4, y: 8, z: 16 (z_hi: 2, z_lo: 8; z = z_hi * 8 + z_lo), core: 2. Of those that a mesh axis runs over, the one named last changes fastest.
Arguments:
- fields: float32 [4, 32, 256, 2048], P(None, 'gx', 'gy', 'gz'), may hold values from 0 to 1
- grain_ids: int32 [32, 256], P('gx', 'gy'), may hold values from 0 to 63
- grain_angle: float32 [64], replicated, may hold values from -3.140625 to 3.140625
- melt_planes: float32 [2, 4, 32, 256, 16], P(None, None, 'gx', 'gy'), may hold values from 0 to 1
- shifts: int32 [2], replicated, may hold values from 1 to 16, as said below
Outputs:
- fields_out: float32 [4, 32, 256, 2048], P(None, 'gx', 'gy', 'gz')
The draws below stay inside these ranges and needn't reach their ends.
Inputs may be any that keep to these rules, and one draw needn't show every extreme that they name: `shifts`: one of the two entries equals 16.
All inputs are finite; a program needn't handle non-finite values.
Results may differ from the reference program's by a relative error of at most 0.0001.
Values sent between devices are 32-bit elements; how exact they have to be, the bound alone decides.
No kernel may reach another device: no remote copies, remote signals or barrier semaphores. Data moves between devices by JAX's collectives and lax.ppermute only.
A program may use at most 32 MiB of HBM per device.

```python
import jax
import jax.numpy as jnp
from jax import lax

STEPS = 4
SHIFT = 16
GRAINS = 64
NX = 32
NY = 256
NZ = 2048


def draw_shifts(key, part):
    first_key, second_key = jax.random.split(key)
    counts = jax.random.randint(first_key, (2,), 1, SHIFT + 1)
    chosen_variant = jax.random.randint(second_key, (), 0, 2)
    return jnp.where(jnp.arange(2) == chosen_variant, SHIFT, counts).astype(jnp.int32)


def touch_ends(drawn, rng, least, high):
    index_at = [jax.random.randint(jax.random.fold_in(rng, axis), (), 0, length) for axis, length in enumerate(drawn.shape)]
    longest = drawn.shape.index(max(drawn.shape))
    neighbour = index_at[:longest] + [(index_at[longest] + 1) % drawn.shape[longest]] + index_at[longest + 1:]
    return drawn.at[tuple(index_at)].set(least).at[tuple(neighbour)].set(high)


def shard_levels(rng, dims, shards, low, largest):
    loudness = 1.0
    for dim, parts in shards:
        heights = jax.random.uniform(jax.random.fold_in(jax.random.fold_in(rng, 6), dim), (parts,), jnp.float32, low / len(shards), largest / len(shards))
        loudness = loudness * jnp.repeat(jnp.exp(heights), dims[dim] // parts).reshape((-1,) + (1,) * (len(dims) - 1 - dim))
    return loudness


def setup_inputs(seed: int = 0) -> dict:
    key_list = jax.random.split(jax.random.key(seed), 6)
    return {
        "fields": jnp.clip(1.0 * jax.random.uniform(key_list[0], (4, NX, NY, NZ), jnp.float32) ** shard_levels(key_list[0], (4, NX, NY, NZ), ((1, 4), (2, 16), (3, 16)), -0.2, 0.2), 0.0, 1.0),
        "grain_ids": touch_ends(jax.random.randint(key_list[1], (NX, NY), 0, GRAINS), jax.random.fold_in(key_list[1], 1), 0, GRAINS - 1).astype(jnp.int32),
        "grain_angle": jnp.clip(jax.random.uniform(key_list[2], (GRAINS,), jnp.float32, -3.140625, 3.140625), -3.140625, 3.140625),
        "melt_planes": jnp.clip(1.0 * jax.random.uniform(key_list[3], (2, 4, NX, NY, SHIFT), jnp.float32) ** shard_levels(key_list[3], (2, 4, NX, NY, SHIFT), ((2, 4), (3, 16)), -0.2, 0.2), 0.0, 1.0),
        "shifts": draw_shifts(jax.random.fold_in(key_list[5], 71), 0),
    }


time_step = 0.05
well_weight = 1.5
grad_weight = 0.05
aniso_weight = 0.6
couple_weights = (0.3, -0.2, 0.1)
solute_slopes = (0.5, 0.8, 1.1)


def laplace(field):
    middle = field[..., 1:-1, 1:-1, 1:-1]
    summed = field[..., 2:, 1:-1, 1:-1] + field[..., :-2, 1:-1, 1:-1]
    summed = summed + field[..., 1:-1, 2:, 1:-1] + field[..., 1:-1, :-2, 1:-1]
    summed = summed + field[..., 1:-1, 1:-1, 2:] + field[..., 1:-1, 1:-1, :-2]
    return summed - 6.0 * middle


def mobility_of(grain_ids, grain_angle):
    number_list = jnp.arange(grain_angle.shape[0], dtype=jnp.int32)
    onehot = (grain_ids[None, :, :] == number_list[:, None, None]).astype(jnp.float32)
    angle_map = jnp.sum(onehot * grain_angle[:, None, None], axis=0)
    return jnp.stack([1.0 + aniso_weight * jnp.cos(4.0 * angle_map + 2.0944 * phase_idx) for phase_idx in range(3)])


def heat_distribution(solidifying_direction, slice_count):
    return (2.0 * solidifying_direction.astype(jnp.float32) + 1.0) / slice_count - 1.0


def step_core(padded, mobility, heat_gradient_curve):
    solute_wide = padded[3]
    potential = solute_wide[1:-1, 1:-1, 1:-1] - grad_weight * laplace(solute_wide)
    for phase_idx in range(3):
        potential = potential + couple_weights[phase_idx] * padded[phase_idx, 1:-1, 1:-1, 1:-1]
    dopant_current = laplace(potential)
    interior = padded[:, 2:-2, 2:-2, 2:-2]
    phases_in = interior[:3]
    solute_in = interior[3]
    phase_lap = laplace(padded[:3, 1:-1, 1:-1, 1:-1])
    squares = jnp.sum(phases_in * phases_in, axis=0)
    results = []
    for phase_idx in range(3):
        value = phases_in[phase_idx]
        well = 2.0 * value * (1.0 - value) * (1.0 - 2.0 * value) + well_weight * value * (squares - value * value)
        drive = 6.0 * value * (1.0 - value) * (heat_gradient_curve + solute_slopes[phase_idx] * (solute_in - 0.5))
        update = mobility[phase_idx][:, :, None] * (phase_lap[phase_idx] - well) - drive
        results.append(value + time_step * update)
    results.append(solute_in + time_step * dopant_current)
    return jnp.stack(results)


def reference(fields, grain_ids, grain_angle, melt_planes, shifts):
    mobility = mobility_of(grain_ids, grain_angle)
    slice_count = fields.shape[3]
    heat_gradient_curve = heat_distribution(jnp.arange(slice_count, dtype=jnp.int32), slice_count)
    for turn_index in range(STEPS):
        padded = jnp.pad(fields, ((0, 0), (2, 2), (2, 2), (0, 0)), mode="wrap")
        padded = jnp.pad(padded, ((0, 0), (0, 0), (0, 0), (2, 2)))
        fields = step_core(padded, mobility, heat_gradient_curve)
        if turn_index % 2 == 1:
            advance = turn_index // 2
            combined = jnp.concatenate([fields, melt_planes[advance]], axis=3)
            fields = lax.dynamic_slice_in_dim(combined, shifts[advance].astype(jnp.int32), slice_count, 3)
    return fields
```

```python
import jax
import jax.numpy as jnp
from jax import lax
from jax.experimental import pallas as pl
from jax.experimental.pallas import tpu as pltpu
from jax.sharding import PartitionSpec as P


f32 = jnp.float32
SLOPES = (0.5, 0.8, 1.1)
ZE = 40

Y_ROWS = 224
Y_MELT, Y_IDS = 208, 218
Z_ROWS = 176
X1_ROWS = 512 + Z_ROWS + 8
Z2_TILES = 18
X2_ROWS = 280


def lanes(shape):
    return lax.broadcasted_iota(jnp.int32, shape, len(shape) - 1)


def subs(shape):
    return lax.broadcasted_iota(jnp.int32, shape, len(shape) - 2)


def three(a, b, c):
    lane = lanes(a.shape)
    out = jnp.where(lane < ZE, a, pltpu.roll(b, ZE, len(a.shape) - 1))
    return out if c is None else jnp.where(lane < 2 * ZE, out, pltpu.roll(c, 2 * ZE, len(a.shape) - 1))


def part(a, group):
    return a if group == 0 else pltpu.roll(a, 128 - ZE * group, len(a.shape) - 1)


def combined(c, p0, p1, p2):
    return c - 6.0 * p0 + 4.0 * p1 - 2.0 * p2


def pack_first(f_in, ids_in, melt_in, up, dn, f, ids, melt, sems):
    copies = [
        pltpu.make_async_copy(f_in, f, sems.at[0]),
        pltpu.make_async_copy(ids_in, ids, sems.at[1]),
        pltpu.make_async_copy(melt_in.at[0], melt, sems.at[2]),
    ]
    for copy in copies:
        copy.start()
    copies[0].wait()
    for x in range(8):
        up[8 * x : 8 * x + 8, :] = f[3, x, 8:16, :]
        up[8 * x : 8 * x + 1, :] = combined(f[3, x, 8:9, :], f[0, x, 9:10, :], f[1, x, 9:10, :], f[2, x, 9:10, :])
        dn[8 * x : 8 * x + 8, :] = f[3, x, 0:8, :]
        dn[8 * x + 7 : 8 * x + 8, :] = combined(f[3, x, 7:8, :], f[0, x, 6:7, :], f[1, x, 6:7, :], f[2, x, 6:7, :])
        for k in range(3):
            at = 64 + 18 * x + 6 * k
            up[at : at + 6, :] = f[k, x, 10:16, :]
            dn[at : at + 6, :] = f[k, x, 0:6, :]

    copies[1].wait()
    copies[2].wait()

    def beside(k, y):
        return jnp.concatenate([melt[k, x, y : y + 1, :] for x in range(8)], axis=1)

    m = Y_MELT
    up[m : m + 1, :] = combined(beside(3, 12), beside(0, 13), beside(1, 13), beside(2, 13))
    dn[m + 3 : m + 4, :] = combined(beside(3, 3), beside(0, 2), beside(1, 2), beside(2, 2))
    for j in range(3):
        up[m + 1 + j : m + 2 + j, :] = beside(3, 13 + j)
        dn[m + j : m + 1 + j, :] = beside(3, j)
    for k in range(3):
        for j in range(2):
            at = m + 4 + 2 * k + j
            up[at : at + 1, :] = beside(k, 14 + j)
            dn[at : at + 1, :] = beside(k, j)
    for out in (up, dn):
        out[Y_IDS : Y_IDS + 1, :] = jnp.concatenate([ids[x : x + 1, :].astype(f32) for x in range(8)], axis=1)
        out[Y_IDS + 1 : Y_ROWS, :] = jnp.zeros((Y_ROWS - Y_IDS - 1, 128), f32)


def pack_low(f, ids, zp, row):
    row[...] = jnp.zeros(row.shape, f32)
    row[0:1, :] = jnp.concatenate([ids[x : x + 1, :].astype(f32) for x in range(8)], axis=1)
    for x in range(8):
        zp[16 * x : 16 * x + 16, :] = three(f[0, x], f[1, x], f[2, x])
    for x in range(3):
        zp[128 + 16 * x : 144 + 16 * x, :] = three(f[3, x], f[3, x + 3], f[3, x + 6] if x < 2 else None)


def mobility_of(grain, angles):
    angle = jnp.zeros(grain.shape, f32)
    for g in range(angles.shape[0]):
        angle = jnp.where(grain == float(g), angles[g], angle)
    return [1.0 + 0.6 * jnp.cos(4.0 * angle + 2.0944 * k) for k in range(3)]


def pack_own(scal, angles, f, ids, z1, meltp, x1, zp, mob):
    mob[...] = jnp.zeros(mob.shape, f32)
    for k, row in enumerate(mobility_of(ids[0:1, :], angles)):
        mob[k : k + 1, :] = row
    top = scal[0] == scal[3] - 1
    own = jnp.where(top, meltp[...], z1[...])
    zp[...] = own
    for k in range(4):
        for x in range(8):
            at = 128 * k + 16 * x
            x1[at : at + 16, :] = f[k, x]
    x1[512 : 512 + Z_ROWS, :] = own
    x1[512 + Z_ROWS :, :] = mob[...]


def columns(mo, src, row, x, X, y, Y, n):
    hit = lanes((n, 128)) == 16 * x + y + subs((n, 128))
    for k in range(3):
        value = jnp.sum(jnp.where(hit, src[row + k : row + k + 1, :], 0.0), axis=1, keepdims=True)
        mo[k, X, Y : Y + n, :] = jnp.broadcast_to(0.05 * value, (n, 128))


def own_columns(mob, mown):
    for x in range(8):
        columns(mown, mob, 0, x, x, 0, 0, 16)


def tiles_of(src, base, side, dst):
    for x in range(8):
        dst[3, side, x] = src[base + 8 * x : base + 8 * x + 8, :]
        for k in range(3):
            at = base + 64 + 18 * x + 6 * k
            dst[k, side, x] = jnp.zeros((8, 128), f32)
            dst[k, side, x, 2 - 2 * side : 8 - 2 * side, :] = src[at : at + 6, :]


def unpack_y(lo, hi, yh, z2):
    tiles_of(lo, 0, 0, yh)
    tiles_of(hi, 0, 1, yh)

    def tile(t):
        return lo[8 * t : 8 * t + 8, :] if t < 26 else hi[8 * (t - 26) : 8 * (t - 26) + 8, :]

    for t in range(Z2_TILES):
        z2[8 * t : 8 * t + 8, :] = three(tile(t), tile(t + 18), tile(t + 36) if t + 36 < 52 else None)


def unpack_z(scal, angles, z2, lo, hi, yh, eh, up, dn, moby, flat):
    moby[...] = jnp.zeros(moby.shape, f32)
    for side, src in ((0, lo), (3, hi)):
        for k, row in enumerate(mobility_of(src[Y_IDS : Y_IDS + 1, :], angles)):
            moby[side + k : side + k + 1, :] = row

    for t in range(Z2_TILES):
        tile = z2[8 * t : 8 * t + 8, :]
        for g in range(3):
            if t + 18 * g < 52:
                flat[8 * (t + 18 * g) : 8 * (t + 18 * g) + 8, :] = part(tile, g)
    tiles_of(flat, 0, 0, eh)
    tiles_of(flat, 208, 1, eh)

    @pl.when(scal[0] == scal[3] - 1)
    def _():
        eh[...] = jnp.zeros(eh.shape, f32)
        for side, src in ((0, lo), (1, hi)):
            for x in range(8):
                rows = src[Y_MELT : Y_MELT + 10, :]
                if x:
                    rows = pltpu.roll(src[Y_MELT : Y_MELT + 16, :], 128 - 16 * x, 1)
                eh[3, side, x, 4 - 4 * side : 8 - 4 * side, :] = rows[0:4]
                for k in range(3):
                    eh[k, side, x, 6 - 6 * side : 8 - 6 * side, :] = rows[4 + 2 * k : 6 + 2 * k]

    sub = subs((8, 128))
    for out, col in ((up, lambda dx: 8 - dx), (dn, lambda dx: dx - 1)):

        def corner(src, k, dx):
            if k == 3:
                return jnp.where(sub >= dx, src[3, 0, col(dx)], src[3, 1, col(8 - dx)])
            return jnp.where(sub > dx, src[k, 0, col(dx)], src[k, 1, col(7 - dx)])

        at = 0
        for dx in range(1, 8):
            out[at : at + 8, :] = corner(yh, 3, dx)
            at += 8
        for k in range(3):
            for dx in range(1, 7):
                out[at : at + 8, :] = corner(yh, k, dx)
                at += 8
        for i in range(3):
            out[at : at + 8, :] = three(corner(eh, 3, 1 + i), corner(eh, 3, 4 + i), corner(eh, 3, 7) if i == 0 else None)
            at += 8
        for dx in range(1, 7):
            out[at : at + 8, :] = three(corner(eh, 0, dx), corner(eh, 1, dx), corner(eh, 2, dx))
            at += 8
        out[at : at + 8, :] = moby[...]


def steps(scal, f, zp, mown, x1lo, x1hi, moby, yh, eh, x2lo, x2hi, out, a, b, u, ex, mo):
    gz, s1, s2, top = scal[0], scal[1], scal[2], scal[0] == scal[3] - 1
    planes = scal[3] * 128

    for k in range(4):
        a[k, 8:16, 8:24, 0:128] = f[k]
        for x in range(8):
            at = 128 * k + 16 * x
            a[k, x, 8:24, 0:128] = x1lo[at : at + 16, :]
            a[k, 16 + x, 8:24, 0:128] = x1hi[at : at + 16, :]
            for src, base, X in ((zp, 0, 8), (x1lo, 512, 0), (x1hi, 512, 16)):
                r = base + (16 * x if k < 3 else 128 + 16 * (x % 3))
                ex[k, X + x, 8:24, :] = part(src[r : r + 16, :], k if k < 3 else x // 3)
        for side in range(2):
            a[k, 8:16, 24 * side : 24 * side + 8, 0:128] = yh[k, side]
            ex[k, 8:16, 24 * side : 24 * side + 8, :] = eh[k, side]
    for src, lo_col, hi_col in ((x2lo, lambda d: 8 - d, lambda d: 8 - d), (x2hi, lambda d: 15 + d, lambda d: 15 + d)):
        for k in (3, 0, 1, 2):
            for dx in range(1, 8 if k == 3 else 7):
                at = 8 * (dx - 1) if k == 3 else 56 + 48 * k + 8 * (dx - 1)
                tile = src[at : at + 8, :]
                if k == 3:
                    above = part(src[200 + 8 * ((dx - 1) % 3) : 208 + 8 * ((dx - 1) % 3), :], (dx - 1) // 3)
                    other = 8 - dx
                else:
                    above = part(src[224 + 8 * (dx - 1) : 232 + 8 * (dx - 1), :], k)
                    other = 7 - dx
                a[k, lo_col(dx), 0:8, 0:128] = tile
                a[k, hi_col(other), 24:32, 0:128] = tile
                ex[k, lo_col(dx), 0:8, :] = above
                ex[k, hi_col(other), 24:32, :] = above

    mo[:, 8:16, 8:24, :] = mown[...]
    for x in range(8):
        columns(mo, moby, 0, x, 8 + x, 8, 0, 8)
        columns(mo, moby, 3, x, 8 + x, 0, 24, 8)
        for src, second, X in ((x1lo, x2lo, x), (x1hi, x2hi, 16 + x)):
            if 3 <= X < 21:
                columns(mo, src, 512 + Z_ROWS, x, X, 0, 8, 16)
                columns(mo, second, 272, x, X, 8, 0, 8)
                columns(mo, second, 275, x, X, 0, 24, 8)

    plane = gz * 128 + lanes((1, 256))
    for k in range(4):
        for X in range(24):
            a[k, X, :, 128:256] = jnp.where(plane[:, 128:] < planes, ex[k, X], 0.0)

    first, second = plane[:, :128], plane[:, 128:]

    def one(src, dst, reach, moved, low, high, rows, melt):
        heat = (2.0 * (plane - moved).astype(f32) + 1.0) / planes.astype(f32) - 1.0
        warm = [0.3 * heat - 0.15 * slope for slope in SLOPES]

        def sides(v):
            return (pltpu.roll(v, 1, 0) + pltpu.roll(v, 31, 0)) + (pltpu.roll(v, 1, 1) + pltpu.roll(v, 255, 1))

        def potential(X, _):
            c = src[3, X]
            around = (src[3, X - 1] + src[3, X + 1]) + sides(c)
            u[X] = 1.3 * c - 0.05 * around + (0.3 * src[0, X] - 0.2 * src[1, X] + 0.1 * src[2, X])
            return _

        lax.fori_loop(8 - reach - 1, 16 + reach + 1, potential, 0)

        def update(X, _):
            v = u[X]
            c = src[3, X]
            around = (u[X - 1] + u[X + 1]) + sides(v)
            new = [None] * 4
            new[3] = c + (0.05 * around - 0.3 * v)
            p = [src[k, X] for k in range(3)]
            sq = [w * w for w in p]
            shared = 8.0 + 1.5 * ((sq[0] + sq[1]) + sq[2])
            for k in range(3):
                w = p[k]
                near = (src[k, X - 1] + src[k, X + 1]) + sides(w)
                rate = mo[k, X]
                rate = jnp.concatenate([rate, rate], axis=1)
                grow = w + rate * (near - w * (shared + w * (2.5 * w - 6.0)))
                new[k] = grow - (w - sq[k]) * (warm[k] + 0.3 * SLOPES[k] * c)
            for k in range(4):
                own, above = new[k][rows, :128], new[k][rows, 128:]
                if low is not None:
                    own = jnp.where(first >= low, own, 0.0)
                if melt:
                    above = jnp.where(top, ex[k, X], above)
                if high is not None:
                    above = jnp.where(second < high, above, 0.0)
                dst[k, X, rows, 0:128] = own
                dst[k, X, rows, 128:256] = above
            return _

        lax.fori_loop(8 - reach, 16 + reach, update, 0)

    every = slice(0, 32)
    one(a, b, 6, 0, None, planes, every, False)
    one(b, a, 4, 0, s1, planes + s1, every, True)
    one(a, b, 2, s1, s1, planes + s1, every, False)
    one(b, a, 0, s1, None, None, slice(8, 24), False)

    total = s1 + s2
    lane = lanes((1, 128))
    for k in range(4):
        for x in range(8):
            melt = pltpu.roll(ex[k, 8 + x, 8:24, :], (s1 + 112) % 128, 1)
            above = a[k, 8 + x, 8:24, 128:256]
            above = jnp.where(top & (lane >= s1), melt, above)
            own = pltpu.roll(a[k, 8 + x, 8:24, 0:128], 128 - total, 1)
            above = pltpu.roll(above, 128 - total, 1)
            out[k, x] = jnp.where(lane < 128 - total, own, above)


def kernel(fn, mib, out_shapes, scratch=(), scalars=0, hbm=False):
    def call(*args):
        specs = [pl.BlockSpec(memory_space=pltpu.HBM if hbm else pltpu.VMEM) for _ in args]
        specs[:scalars] = [pl.BlockSpec(memory_space=pltpu.SMEM)] * scalars
        return pl.pallas_call(
            fn,
            in_specs=specs,
            out_specs=[pl.BlockSpec(memory_space=pltpu.VMEM) for _ in out_shapes],
            out_shape=[jax.ShapeDtypeStruct(s, f32) for s in out_shapes],
            scratch_shapes=[pltpu.VMEM(s, f32) if isinstance(s, tuple) else s for s in scratch],
            compiler_params=pltpu.CompilerParams(vmem_limit_bytes=mib if mib > 1000 else mib << 20),
        )(*args)

    return call


def ring(value, axis, by):
    n = lax.axis_size(axis)
    return lax.ppermute(value, axis, [(i, (i + by) % n) for i in range(n)])


def from_above(value):
    n = lax.axis_size("gz")
    return lax.ppermute(value, "gz", [(i, i - 1) for i in range(1, n)])


def melt_above(melt):
    both = jnp.concatenate([melt[0], melt[1], jnp.zeros(melt.shape[1:4] + (ZE - 32,), f32)], axis=-1)
    phases = jnp.pad(jnp.concatenate([both[0], both[1], both[2]], axis=-1).reshape(128, 3 * ZE), ((0, 0), (0, 8)))
    c = jnp.pad(both[3], ((0, 1), (0, 0), (0, 0)))
    solute = jnp.pad(jnp.concatenate([c[0:3], c[3:6], c[6:9]], axis=-1).reshape(48, 3 * ZE), ((0, 0), (0, 8)))
    return jnp.concatenate([phases, solute], axis=0)


def body(fields, grain_ids, grain_angle, melt_planes, shifts):
    inputs = [fields.shape, pltpu.VMEM(grain_ids.shape, jnp.int32), melt_planes.shape[1:], pltpu.SemaphoreType.DMA((3,))]
    up, dn = kernel(pack_first, 4, [(Y_ROWS, 128)] * 2, inputs, hbm=True)(fields, grain_ids, melt_planes)
    ylo = ring(up, "gy", 1)
    yhi = ring(dn, "gy", -1)
    low, ids = kernel(pack_low, 2, [(Z_ROWS, 128), (8, 128)])(fields, grain_ids)
    z1 = from_above(low)
    gz = lax.axis_index("gz").astype(jnp.int32)
    scal = jnp.stack([gz, shifts[0], shifts[1], jnp.int32(lax.axis_size("gz"))])
    x1, zp, mob = kernel(pack_own, 2, [(X1_ROWS, 128), (Z_ROWS, 128), (8, 128)], scalars=2)(
        scal, grain_angle, fields, ids, z1, melt_above(melt_planes)
    )
    (mown,) = kernel(own_columns, 2, [(3, 8, 16, 128)])(mob)
    x1lo = ring(x1, "gx", 1)
    x1hi = ring(x1, "gx", -1)
    tiles = (4, 2, 8, 8, 128)
    yh, z2 = kernel(unpack_y, 2, [tiles, (8 * Z2_TILES, 128)])(ylo, yhi)
    z2 = from_above(z2)
    shapes = [tiles, (X2_ROWS, 128), (X2_ROWS, 128), (8, 128)]
    eh, up2, dn2, moby = kernel(unpack_z, 4, shapes, [(416, 128)], scalars=2)(scal, grain_angle, z2, ylo, yhi, yh)
    x2lo = ring(up2, "gx", 1)
    x2hi = ring(dn2, "gx", -1)
    block = (4, 24, 32, 256)
    (out,) = kernel(
        steps, 24, [(4, 8, 16, 128)], [block, block, block[1:], (4, 24, 32, 128), (3, 24, 32, 128)], scalars=1
    )(scal, fields, zp, mown, x1lo, x1hi, moby, yh, eh, x2lo, x2hi)
    return out


def solution(mesh):
    placed = (P(None, "gx", "gy", "gz"), P("gx", "gy"), P(), P(None, None, "gx", "gy", None), P())
    return jax.shard_map(
        body, mesh=mesh, in_specs=placed, out_specs=P(None, "gx", "gy", "gz"), check_vma=False
    )
```

```python
import jax
import jax.numpy as jnp
from jax import lax
from jax.experimental import pallas as pl
from jax.experimental.pallas import tpu as pltpu
from jax.sharding import PartitionSpec as P


f32 = jnp.float32
SLOPES = (0.5, 0.8, 1.1)
ZE = 40

Y_ROWS = 224
Y_MELT, Y_IDS = 208, 218
Z_ROWS = 176
Z2_TILES = 18
X2_ZP, X2_MOB = 272, 272 + Z_ROWS
X2_ROWS = X2_MOB + 16


def lanes(shape):
    return lax.broadcasted_iota(jnp.int32, shape, len(shape) - 1)


def subs(shape):
    return lax.broadcasted_iota(jnp.int32, shape, len(shape) - 2)


def three(a, b, c):
    lane = lanes(a.shape)
    out = jnp.where(lane < ZE, a, pltpu.roll(b, ZE, len(a.shape) - 1))
    return out if c is None else jnp.where(lane < 2 * ZE, out, pltpu.roll(c, 2 * ZE, len(a.shape) - 1))


def part(a, group):
    return a if group == 0 else pltpu.roll(a, 128 - ZE * group, len(a.shape) - 1)


def combined(c, p0, p1, p2):
    return c - 6.0 * p0 + 4.0 * p1 - 2.0 * p2


def pack_first(f_in, ids_in, melt_in, up, dn, f, ids, melt, sems):
    copies = [
        pltpu.make_async_copy(f_in, f, sems.at[0]),
        pltpu.make_async_copy(ids_in, ids, sems.at[1]),
        pltpu.make_async_copy(melt_in.at[0], melt, sems.at[2]),
    ]
    for copy in copies:
        copy.start()
    copies[0].wait()
    for x in range(8):
        up[8 * x : 8 * x + 8, :] = f[3, x, 8:16, :]
        up[8 * x : 8 * x + 1, :] = combined(f[3, x, 8:9, :], f[0, x, 9:10, :], f[1, x, 9:10, :], f[2, x, 9:10, :])
        dn[8 * x : 8 * x + 8, :] = f[3, x, 0:8, :]
        dn[8 * x + 7 : 8 * x + 8, :] = combined(f[3, x, 7:8, :], f[0, x, 6:7, :], f[1, x, 6:7, :], f[2, x, 6:7, :])
        for k in range(3):
            at = 64 + 18 * x + 6 * k
            up[at : at + 6, :] = f[k, x, 10:16, :]
            dn[at : at + 6, :] = f[k, x, 0:6, :]

    copies[1].wait()
    copies[2].wait()

    def beside(k, y):
        return jnp.concatenate([melt[k, x, y : y + 1, :] for x in range(8)], axis=1)

    m = Y_MELT
    up[m : m + 1, :] = combined(beside(3, 12), beside(0, 13), beside(1, 13), beside(2, 13))
    dn[m + 3 : m + 4, :] = combined(beside(3, 3), beside(0, 2), beside(1, 2), beside(2, 2))
    for j in range(3):
        up[m + 1 + j : m + 2 + j, :] = beside(3, 13 + j)
        dn[m + j : m + 1 + j, :] = beside(3, j)
    for k in range(3):
        for j in range(2):
            at = m + 4 + 2 * k + j
            up[at : at + 1, :] = beside(k, 14 + j)
            dn[at : at + 1, :] = beside(k, j)
    for out in (up, dn):
        out[Y_IDS : Y_IDS + 1, :] = jnp.concatenate([ids[x : x + 1, :].astype(f32) for x in range(8)], axis=1)
        out[Y_IDS + 1 : Y_ROWS, :] = jnp.zeros((Y_ROWS - Y_IDS - 1, 128), f32)


def pack_low(f, zp, own):
    own[...] = f[...]
    for x in range(8):
        zp[16 * x : 16 * x + 16, :] = three(f[0, x], f[1, x], f[2, x])
    for x in range(3):
        zp[128 + 16 * x : 144 + 16 * x, :] = three(f[3, x], f[3, x + 3], f[3, x + 6] if x < 2 else None)


def mobility_of(grain, angles):
    angle = jnp.zeros(grain.shape, f32)
    for g in range(angles.shape[0]):
        angle = jnp.where(grain == float(g), angles[g], angle)
    return [1.0 + 0.6 * jnp.cos(4.0 * angle + 2.0944 * k) for k in range(3)]


def columns(mo, src, row, x, X, y, Y, n):
    hit = lanes((n, 128)) == 16 * x + y + subs((n, 128))
    for k in range(3):
        value = jnp.sum(jnp.where(hit, src[row + k : row + k + 1, :], 0.0), axis=1, keepdims=True)
        mo[k, X, Y : Y + n, :] = jnp.broadcast_to(0.05 * value, (n, 128))


def own_columns(angles, ids, mob, mown):
    grain = jnp.concatenate([ids[x : x + 1, :].astype(f32) for x in range(8)], axis=1)
    mob[...] = jnp.zeros(mob.shape, f32)
    for k, row in enumerate(mobility_of(grain, angles)):
        mob[k : k + 1, :] = row
    for x in range(8):
        columns(mown, mob, 0, x, x, 0, 0, 16)


def tiles_of(src, base, side, dst):
    for x in range(8):
        dst[3, side, x] = src[base + 8 * x : base + 8 * x + 8, :]
        for k in range(3):
            at = base + 64 + 18 * x + 6 * k
            dst[k, side, x] = jnp.zeros((8, 128), f32)
            dst[k, side, x, 2 - 2 * side : 8 - 2 * side, :] = src[at : at + 6, :]


def unpack_y(lo, hi, yh, z2):
    tiles_of(lo, 0, 0, yh)
    tiles_of(hi, 0, 1, yh)

    def tile(t):
        return lo[8 * t : 8 * t + 8, :] if t < 26 else hi[8 * (t - 26) : 8 * (t - 26) + 8, :]

    for t in range(Z2_TILES):
        z2[8 * t : 8 * t + 8, :] = three(tile(t), tile(t + 18), tile(t + 36) if t + 36 < 52 else None)


def unpack_z(scal, angles, z1, meltp, mob, z2, lo, hi, yh, zp, eh, up, dn, moby, flat):
    top = scal[0] == scal[3] - 1
    zp[...] = jnp.where(top, meltp[...], z1[...])
    moby[...] = jnp.zeros(moby.shape, f32)
    for side, src in ((0, lo), (3, hi)):
        for k, row in enumerate(mobility_of(src[Y_IDS : Y_IDS + 1, :], angles)):
            moby[side + k : side + k + 1, :] = row

    for t in range(Z2_TILES):
        tile = z2[8 * t : 8 * t + 8, :]
        for g in range(3):
            if t + 18 * g < 52:
                flat[8 * (t + 18 * g) : 8 * (t + 18 * g) + 8, :] = part(tile, g)
    tiles_of(flat, 0, 0, eh)
    tiles_of(flat, 208, 1, eh)

    @pl.when(top)
    def _():
        eh[...] = jnp.zeros(eh.shape, f32)
        for side, src in ((0, lo), (1, hi)):
            for x in range(8):
                rows = src[Y_MELT : Y_MELT + 10, :]
                if x:
                    rows = pltpu.roll(src[Y_MELT : Y_MELT + 16, :], 128 - 16 * x, 1)
                eh[3, side, x, 4 - 4 * side : 8 - 4 * side, :] = rows[0:4]
                for k in range(3):
                    eh[k, side, x, 6 - 6 * side : 8 - 6 * side, :] = rows[4 + 2 * k : 6 + 2 * k]

    sub = subs((8, 128))
    for out, col in ((up, lambda dx: 8 - dx), (dn, lambda dx: dx - 1)):

        def corner(src, k, dx):
            if k == 3:
                return jnp.where(sub >= dx, src[3, 0, col(dx)], src[3, 1, col(8 - dx)])
            return jnp.where(sub > dx, src[k, 0, col(dx)], src[k, 1, col(7 - dx)])

        at = 0
        for dx in range(1, 8):
            out[at : at + 8, :] = corner(yh, 3, dx)
            at += 8
        for k in range(3):
            for dx in range(1, 7):
                out[at : at + 8, :] = corner(yh, k, dx)
                at += 8
        for i in range(3):
            out[at : at + 8, :] = three(corner(eh, 3, 1 + i), corner(eh, 3, 4 + i), corner(eh, 3, 7) if i == 0 else None)
            at += 8
        for dx in range(1, 7):
            out[at : at + 8, :] = three(corner(eh, 0, dx), corner(eh, 1, dx), corner(eh, 2, dx))
            at += 8
        out[X2_ZP:X2_MOB, :] = zp[...]
        out[X2_MOB : X2_MOB + 8, :] = moby[...]
        out[X2_MOB + 8 :, :] = mob[...]


def steps(scal, f, zp, mown, x1lo, x1hi, moby, yh, eh, x2lo, x2hi, out, a0, a1, b0, b1, u0, u1, ex, mo):
    gz, s1, s2, top = scal[0], scal[1], scal[2], scal[0] == scal[3] - 1
    planes = scal[3] * 128

    for k in range(4):
        a0[k, 8:16, 8:24, :] = f[k]
        for x in range(8):
            a0[k, x, 8:24, :] = x1lo[k, x]
            a0[k, 16 + x, 8:24, :] = x1hi[k, x]
            for src, base, X in ((zp, 0, 8), (x2lo, X2_ZP, 0), (x2hi, X2_ZP, 16)):
                r = base + (16 * x if k < 3 else 128 + 16 * (x % 3))
                ex[k, X + x, 8:24, :] = part(src[r : r + 16, :], k if k < 3 else x // 3)
        for side in range(2):
            a0[k, 8:16, 24 * side : 24 * side + 8, :] = yh[k, side]
            ex[k, 8:16, 24 * side : 24 * side + 8, :] = eh[k, side]
    for src, lo_col, hi_col in ((x2lo, lambda d: 8 - d, lambda d: 8 - d), (x2hi, lambda d: 15 + d, lambda d: 15 + d)):
        for k in (3, 0, 1, 2):
            for dx in range(1, 8 if k == 3 else 7):
                at = 8 * (dx - 1) if k == 3 else 56 + 48 * k + 8 * (dx - 1)
                tile = src[at : at + 8, :]
                if k == 3:
                    above = part(src[200 + 8 * ((dx - 1) % 3) : 208 + 8 * ((dx - 1) % 3), :], (dx - 1) // 3)
                    other = 8 - dx
                else:
                    above = part(src[224 + 8 * (dx - 1) : 232 + 8 * (dx - 1), :], k)
                    other = 7 - dx
                a0[k, lo_col(dx), 0:8, :] = tile
                a0[k, hi_col(other), 24:32, :] = tile
                ex[k, lo_col(dx), 0:8, :] = above
                ex[k, hi_col(other), 24:32, :] = above

    mo[:, 8:16, 8:24, :] = mown[...]
    for x in range(8):
        columns(mo, moby, 0, x, 8 + x, 8, 0, 8)
        columns(mo, moby, 3, x, 8 + x, 0, 24, 8)
        for src, X in ((x2lo, x), (x2hi, 16 + x)):
            if 3 <= X < 21:
                columns(mo, src, X2_MOB + 8, x, X, 0, 8, 16)
                columns(mo, src, X2_MOB, x, X, 8, 0, 8)
                columns(mo, src, X2_MOB + 3, x, X, 0, 24, 8)

    lane = lanes((8, 128))
    first = gz * 128 + lane
    second = first + 128
    for k in range(4):
        for X in range(24):
            for s in range(0, 32, 8):
                a1[k, X, s : s + 8, :] = jnp.where(second < planes, ex[k, X, s : s + 8, :], 0.0)

    def beside_z(m, e):
        m1, e1, m9, e9 = pltpu.roll(m, 1, 1), pltpu.roll(e, 1, 1), pltpu.roll(m, 127, 1), pltpu.roll(e, 127, 1)
        return m1 + jnp.where(lane == 127, e9, m9), jnp.where(lane == 0, m1, e1) + e9

    def beside_xy(ref, pre, X, s, v):
        low = pltpu.roll(v, 1, 0) if s == 0 else ref[(*pre, X, slice(s - 1, s + 7))]
        across = ref[(*pre, X - 1, slice(s, s + 8))] + ref[(*pre, X + 1, slice(s, s + 8))]
        return across + (low + ref[(*pre, X, slice(s + 1, s + 9))])

    def both(refs, pre, X, s):
        m, e = refs[0][(*pre, X, slice(s, s + 8))], refs[1][(*pre, X, slice(s, s + 8))]
        zm, ze = beside_z(m, e)
        return (m, beside_xy(refs[0], pre, X, s, m) + zm), (e, beside_xy(refs[1], pre, X, s, e) + ze)

    def one(src, dst, reach, moved, low, high, melt, u_tiles, tiles):
        warm = []
        for plane in (first, second):
            heat = (2.0 * (plane - moved).astype(f32) + 1.0) / planes.astype(f32) - 1.0
            warm.append([0.3 * heat - 0.15 * slope for slope in SLOPES])

        def potential(X, s):
            for half, (c, around) in enumerate(both(src, (3,), X, s)):
                p = [src[half][k, X, s : s + 8, :] for k in range(3)]
                value = (1.3 * c - 0.05 * around) + (0.3 * p[0] - 0.2 * p[1] + 0.1 * p[2])
                (u0, u1)[half][X, s : s + 8, :] = value

        def update(X, s):
            rows = slice(s, s + 8)
            flow = both((u0, u1), (), X, s)
            phases = [both(src, (k,), X, s) for k in range(3)]
            rates = [mo[k, X, rows, :] for k in range(3)]
            for half in range(2):
                c = src[half][3, X, rows, :]
                v, around = flow[half]
                new = [None, None, None, c + (0.05 * around - 0.3 * v)]
                sq = [w * w for w, _ in (p[half] for p in phases)]
                shared = 8.0 + 1.5 * ((sq[0] + sq[1]) + sq[2])
                for k in range(3):
                    w, near = phases[k][half]
                    grow = w + rates[k] * (near - w * (shared + w * (2.5 * w - 6.0)))
                    new[k] = grow - (w - sq[k]) * (warm[half][k] + 0.3 * SLOPES[k] * c)
                for k in range(4):
                    value = new[k]
                    if half == 0 and low is not None:
                        value = jnp.where(first >= low, value, 0.0)
                    if half == 1 and melt:
                        value = jnp.where(top, ex[k, X, rows, :], value)
                    if half == 1 and high is not None:
                        value = jnp.where(second < high, value, 0.0)
                    dst[half][k, X, rows, :] = value

        for X in range(7 - reach, 10 - reach):
            for s in u_tiles:
                potential(X, s)

        def row(X, carry):
            for ahead in u_tiles:
                potential(X + 2, ahead)
            for s in tiles:
                update(X, s)
            return carry

        lax.fori_loop(8 - reach, 16 + reach, row, 0, unroll=4)

    a, b = (a0, a1), (b0, b1)
    every = (0, 8, 16, 24)
    one(a, b, 6, 0, None, planes, False, every, every)
    one(b, a, 4, 0, s1, planes + s1, True, every, (4, 12, 20))
    one(a, b, 2, s1, s1, planes + s1, False, (5, 13, 21), (6, 14, 22))
    one(b, a, 0, s1, None, None, False, (7, 15, 23), (8, 16))

    total = s1 + s2
    for k in range(4):
        for x in range(8):
            for s in (0, 8):
                rows = slice(8 + s, 16 + s)
                melt = pltpu.roll(ex[k, 8 + x, rows, :], (s1 + 112) % 128, 1)
                above = jnp.where(top & (lane >= s1), melt, a1[k, 8 + x, rows, :])
                own = pltpu.roll(a0[k, 8 + x, rows, :], 128 - total, 1)
                above = pltpu.roll(above, 128 - total, 1)
                out[k, x, s : s + 8, :] = jnp.where(lane < 128 - total, own, above)


def kernel(fn, mib, out_shapes, scratch=(), scalars=0, hbm=False):
    def call(*args):
        specs = [pl.BlockSpec(memory_space=pltpu.HBM if hbm else pltpu.VMEM) for _ in args]
        specs[:scalars] = [pl.BlockSpec(memory_space=pltpu.SMEM)] * scalars
        return pl.pallas_call(
            fn,
            in_specs=specs,
            out_specs=[pl.BlockSpec(memory_space=pltpu.VMEM) for _ in out_shapes],
            out_shape=[jax.ShapeDtypeStruct(s, f32) for s in out_shapes],
            scratch_shapes=[pltpu.VMEM(s, f32) if isinstance(s, tuple) else s for s in scratch],
            compiler_params=pltpu.CompilerParams(vmem_limit_bytes=mib if mib > 1000 else mib << 20),
        )(*args)

    return call


def ring(value, axis, by):
    n = lax.axis_size(axis)
    return lax.ppermute(value, axis, [(i, (i + by) % n) for i in range(n)])


def from_above(value):
    n = lax.axis_size("gz")
    return lax.ppermute(value, "gz", [(i, i - 1) for i in range(1, n)])


def melt_above(melt):
    both = jnp.concatenate([melt[0], melt[1], jnp.zeros(melt.shape[1:4] + (ZE - 32,), f32)], axis=-1)
    phases = jnp.pad(jnp.concatenate([both[0], both[1], both[2]], axis=-1).reshape(128, 3 * ZE), ((0, 0), (0, 8)))
    c = jnp.pad(both[3], ((0, 1), (0, 0), (0, 0)))
    solute = jnp.pad(jnp.concatenate([c[0:3], c[3:6], c[6:9]], axis=-1).reshape(48, 3 * ZE), ((0, 0), (0, 8)))
    return jnp.concatenate([phases, solute], axis=0)


def body(fields, grain_ids, grain_angle, melt_planes, shifts):
    inputs = [fields.shape, pltpu.VMEM(grain_ids.shape, jnp.int32), melt_planes.shape[1:], pltpu.SemaphoreType.DMA((3,))]
    up, dn = kernel(pack_first, 4, [(Y_ROWS, 128)] * 2, inputs, hbm=True)(
        fields, pltpu.with_memory_space_constraint(grain_ids, pltpu.HBM), pltpu.with_memory_space_constraint(melt_planes, pltpu.HBM)
    )
    ylo = ring(up, "gy", 1)
    yhi = ring(dn, "gy", -1)
    x1lo = ring(fields, "gx", 1)
    x1hi = ring(fields, "gx", -1)
    low, own = kernel(pack_low, 2, [(Z_ROWS, 128), fields.shape])(fields)
    z1 = from_above(low)
    gz = lax.axis_index("gz").astype(jnp.int32)
    scal = jnp.stack([gz, shifts[0], shifts[1], jnp.int32(lax.axis_size("gz"))])
    mob, mown = kernel(own_columns, 2, [(8, 128), (3, 8, 16, 128)], scalars=1)(grain_angle, grain_ids)
    tiles = (4, 2, 8, 8, 128)
    yh, z2 = kernel(unpack_y, 2, [tiles, (8 * Z2_TILES, 128)])(ylo, yhi)
    z2 = from_above(z2)
    shapes = [(Z_ROWS, 128), tiles, (X2_ROWS, 128), (X2_ROWS, 128), (8, 128)]
    zp, eh, up2, dn2, moby = kernel(unpack_z, 4, shapes, [(416, 128)], scalars=2)(
        scal, grain_angle, z1, melt_above(melt_planes), mob, z2, ylo, yhi, yh
    )
    x2lo = ring(up2, "gx", 1)
    x2hi = ring(dn2, "gx", -1)
    block = (4, 26, 40, 128)
    (out,) = kernel(
        steps, 24, [(4, 8, 16, 128)], [block] * 4 + [block[1:]] * 2 + [(4, 24, 32, 128), (3, 24, 32, 128)], scalars=1
    )(scal, own, zp, mown, x1lo, x1hi, moby, yh, eh, x2lo, x2hi)
    return out


def solution(mesh):
    placed = (P(None, "gx", "gy", "gz"), P("gx", "gy"), P(), P(None, None, "gx", "gy", None), P())
    return jax.shard_map(
        body, mesh=mesh, in_specs=placed, out_specs=P(None, "gx", "gy", "gz"), check_vma=False
    )
```

```python
import functools

import jax
import jax.numpy as jnp
from jax import lax
from jax.experimental import pallas as pl
from jax.experimental.pallas import tpu as pltpu
from jax.sharding import PartitionSpec as P


f32 = jnp.float32
SLOPES = (0.5, 0.8, 1.1)
ZE = 40

Y_ROWS = 224
Y_MELT, Y_IDS = 208, 218
Z_ROWS = 176
Z2_TILES = 18
X2_ZP, X2_MOB = 272, 272 + Z_ROWS
X2_ROWS = X2_MOB + 16


def lanes(shape):
    return lax.broadcasted_iota(jnp.int32, shape, len(shape) - 1)


def subs(shape):
    return lax.broadcasted_iota(jnp.int32, shape, len(shape) - 2)


def three(a, b, c):
    lane = lanes(a.shape)
    out = jnp.where(lane < ZE, a, pltpu.roll(b, ZE, len(a.shape) - 1))
    return out if c is None else jnp.where(lane < 2 * ZE, out, pltpu.roll(c, 2 * ZE, len(a.shape) - 1))


def part(a, group):
    return a if group == 0 else pltpu.roll(a, 128 - ZE * group, len(a.shape) - 1)


def combined(c, p0, p1, p2):
    return c - 6.0 * p0 + 4.0 * p1 - 2.0 * p2


def pack_first(f_in, ids_in, melt_in, up, dn, f, ids, melt, sems):
    copies = [
        pltpu.make_async_copy(f_in, f, sems.at[0]),
        pltpu.make_async_copy(ids_in, ids, sems.at[1]),
        pltpu.make_async_copy(melt_in.at[0], melt, sems.at[2]),
    ]
    for copy in copies:
        copy.start()
    copies[0].wait()
    for x in range(8):
        up[8 * x : 8 * x + 8, :] = f[3, x, 8:16, :]
        up[8 * x : 8 * x + 1, :] = combined(f[3, x, 8:9, :], f[0, x, 9:10, :], f[1, x, 9:10, :], f[2, x, 9:10, :])
        dn[8 * x : 8 * x + 8, :] = f[3, x, 0:8, :]
        dn[8 * x + 7 : 8 * x + 8, :] = combined(f[3, x, 7:8, :], f[0, x, 6:7, :], f[1, x, 6:7, :], f[2, x, 6:7, :])
        for k in range(3):
            at = 64 + 18 * x + 6 * k
            up[at : at + 6, :] = f[k, x, 10:16, :]
            dn[at : at + 6, :] = f[k, x, 0:6, :]

    copies[1].wait()
    copies[2].wait()

    def beside(k, y):
        return jnp.concatenate([melt[k, x, y : y + 1, :] for x in range(8)], axis=1)

    m = Y_MELT
    up[m : m + 1, :] = combined(beside(3, 12), beside(0, 13), beside(1, 13), beside(2, 13))
    dn[m + 3 : m + 4, :] = combined(beside(3, 3), beside(0, 2), beside(1, 2), beside(2, 2))
    for j in range(3):
        up[m + 1 + j : m + 2 + j, :] = beside(3, 13 + j)
        dn[m + j : m + 1 + j, :] = beside(3, j)
    for k in range(3):
        for j in range(2):
            at = m + 4 + 2 * k + j
            up[at : at + 1, :] = beside(k, 14 + j)
            dn[at : at + 1, :] = beside(k, j)
    for out in (up, dn):
        out[Y_IDS : Y_IDS + 1, :] = jnp.concatenate([ids[x : x + 1, :].astype(f32) for x in range(8)], axis=1)
        out[Y_IDS + 1 : Y_ROWS, :] = jnp.zeros((Y_ROWS - Y_IDS - 1, 128), f32)


def pack_low(f, zp):
    for x in range(8):
        zp[16 * x : 16 * x + 16, :] = three(f[0, x], f[1, x], f[2, x])
    for x in range(3):
        zp[128 + 16 * x : 144 + 16 * x, :] = three(f[3, x], f[3, x + 3], f[3, x + 6] if x < 2 else None)


def mobility_of(grain, angles):
    angle = jnp.zeros(grain.shape, f32)
    for g in range(angles.shape[0]):
        angle = jnp.where(grain == float(g), angles[g], angle)
    return [1.0 + 0.6 * jnp.cos(4.0 * angle + 2.0944 * k) for k in range(3)]


def columns(mo, src, row, x, X, y, Y, n):
    hit = lanes((n, 128)) == 16 * x + y + subs((n, 128))
    for k in range(3):
        value = jnp.sum(jnp.where(hit, src[row + k : row + k + 1, :], 0.0), axis=1, keepdims=True)
        mo[k, X, Y : Y + n, :] = jnp.broadcast_to(0.05 * value, (n, 128))


def own_columns(angles, ids, mob, mown):
    grain = jnp.concatenate([ids[x : x + 1, :].astype(f32) for x in range(8)], axis=1)
    mob[...] = jnp.zeros(mob.shape, f32)
    for k, row in enumerate(mobility_of(grain, angles)):
        mob[k : k + 1, :] = row
    for x in range(8):
        columns(mown, mob, 0, x, x, 0, 0, 16)


def tiles_of(src, base, side, dst):
    for x in range(8):
        dst[3, side, x] = src[base + 8 * x : base + 8 * x + 8, :]
        for k in range(3):
            at = base + 64 + 18 * x + 6 * k
            dst[k, side, x] = jnp.zeros((8, 128), f32)
            dst[k, side, x, 2 - 2 * side : 8 - 2 * side, :] = src[at : at + 6, :]


def unpack_y(lo, hi, yh, z2):
    tiles_of(lo, 0, 0, yh)
    tiles_of(hi, 0, 1, yh)

    def tile(t):
        return lo[8 * t : 8 * t + 8, :] if t < 26 else hi[8 * (t - 26) : 8 * (t - 26) + 8, :]

    for t in range(Z2_TILES):
        z2[8 * t : 8 * t + 8, :] = three(tile(t), tile(t + 18), tile(t + 36) if t + 36 < 52 else None)


def unpack_z(scal, angles, z1, meltp, mob, z2, lo, hi, yh, zp, eh, up, dn, moby, flat):
    top = scal[0] == scal[3] - 1
    zp[...] = jnp.where(top, meltp[...], z1[...])
    moby[...] = jnp.zeros(moby.shape, f32)
    for side, src in ((0, lo), (3, hi)):
        for k, row in enumerate(mobility_of(src[Y_IDS : Y_IDS + 1, :], angles)):
            moby[side + k : side + k + 1, :] = row

    for t in range(Z2_TILES):
        tile = z2[8 * t : 8 * t + 8, :]
        for g in range(3):
            if t + 18 * g < 52:
                flat[8 * (t + 18 * g) : 8 * (t + 18 * g) + 8, :] = part(tile, g)
    tiles_of(flat, 0, 0, eh)
    tiles_of(flat, 208, 1, eh)

    @pl.when(top)
    def _():
        eh[...] = jnp.zeros(eh.shape, f32)
        for side, src in ((0, lo), (1, hi)):
            for x in range(8):
                rows = src[Y_MELT : Y_MELT + 10, :]
                if x:
                    rows = pltpu.roll(src[Y_MELT : Y_MELT + 16, :], 128 - 16 * x, 1)
                eh[3, side, x, 4 - 4 * side : 8 - 4 * side, :] = rows[0:4]
                for k in range(3):
                    eh[k, side, x, 6 - 6 * side : 8 - 6 * side, :] = rows[4 + 2 * k : 6 + 2 * k]

    sub = subs((8, 128))
    for out, col in ((up, lambda dx: 8 - dx), (dn, lambda dx: dx - 1)):

        def corner(src, k, dx):
            if k == 3:
                return jnp.where(sub >= dx, src[3, 0, col(dx)], src[3, 1, col(8 - dx)])
            return jnp.where(sub > dx, src[k, 0, col(dx)], src[k, 1, col(7 - dx)])

        at = 0
        for dx in range(1, 8):
            out[at : at + 8, :] = corner(yh, 3, dx)
            at += 8
        for k in range(3):
            for dx in range(1, 7):
                out[at : at + 8, :] = corner(yh, k, dx)
                at += 8
        for i in range(3):
            out[at : at + 8, :] = three(corner(eh, 3, 1 + i), corner(eh, 3, 4 + i), corner(eh, 3, 7) if i == 0 else None)
            at += 8
        for dx in range(1, 7):
            out[at : at + 8, :] = three(corner(eh, 0, dx), corner(eh, 1, dx), corner(eh, 2, dx))
            at += 8
        out[X2_ZP:X2_MOB, :] = zp[...]
        out[X2_MOB : X2_MOB + 8, :] = moby[...]
        out[X2_MOB + 8 :, :] = mob[...]


def steps(scal, f, zp, mown, x1lo, x1hi, moby, yh, eh, x2lo, x2hi, out, a0, a1, b0, b1, u0, u1, ex, mo):
    gz, s1, s2, top = scal[0], scal[1], scal[2], scal[0] == scal[3] - 1
    planes = scal[3] * 128

    for k in range(4):
        a0[k, 8:16, 8:24, :] = f[k]
        for x in range(8):
            a0[k, x, 8:24, :] = x1lo[k, x]
            a0[k, 16 + x, 8:24, :] = x1hi[k, x]
            for src, base, X in ((zp, 0, 8), (x2lo, X2_ZP, 0), (x2hi, X2_ZP, 16)):
                r = base + (16 * x if k < 3 else 128 + 16 * (x % 3))
                ex[k, X + x, 8:24, :] = part(src[r : r + 16, :], k if k < 3 else x // 3)
        for side in range(2):
            a0[k, 8:16, 24 * side : 24 * side + 8, :] = yh[k, side]
            ex[k, 8:16, 24 * side : 24 * side + 8, :] = eh[k, side]
    for src, lo_col, hi_col in ((x2lo, lambda d: 8 - d, lambda d: 8 - d), (x2hi, lambda d: 15 + d, lambda d: 15 + d)):
        for k in (3, 0, 1, 2):
            for dx in range(1, 8 if k == 3 else 7):
                at = 8 * (dx - 1) if k == 3 else 56 + 48 * k + 8 * (dx - 1)
                tile = src[at : at + 8, :]
                if k == 3:
                    above = part(src[200 + 8 * ((dx - 1) % 3) : 208 + 8 * ((dx - 1) % 3), :], (dx - 1) // 3)
                    other = 8 - dx
                else:
                    above = part(src[224 + 8 * (dx - 1) : 232 + 8 * (dx - 1), :], k)
                    other = 7 - dx
                a0[k, lo_col(dx), 0:8, :] = tile
                a0[k, hi_col(other), 24:32, :] = tile
                ex[k, lo_col(dx), 0:8, :] = above
                ex[k, hi_col(other), 24:32, :] = above

    mo[:, 8:16, 8:24, :] = mown[...]
    for x in range(8):
        columns(mo, moby, 0, x, 8 + x, 8, 0, 8)
        columns(mo, moby, 3, x, 8 + x, 0, 24, 8)
        for src, X in ((x2lo, x), (x2hi, 16 + x)):
            if 3 <= X < 21:
                columns(mo, src, X2_MOB + 8, x, X, 0, 8, 16)
                columns(mo, src, X2_MOB, x, X, 8, 0, 8)
                columns(mo, src, X2_MOB + 3, x, X, 0, 24, 8)

    lane = lanes((8, 128))
    first = gz * 128 + lane
    second = first + 128
    for k in range(4):
        for X in range(24):
            for s in range(0, 32, 8):
                a1[k, X, s : s + 8, :] = jnp.where(second < planes, ex[k, X, s : s + 8, :], 0.0)

    def beside_z(m, e):
        m1, e1, m9, e9 = pltpu.roll(m, 1, 1), pltpu.roll(e, 1, 1), pltpu.roll(m, 127, 1), pltpu.roll(e, 127, 1)
        return m1 + jnp.where(lane == 127, e9, m9), jnp.where(lane == 0, m1, e1) + e9

    def beside_xy(ref, pre, X, s, v):
        low = pltpu.roll(v, 1, 0) if s == 0 else ref[(*pre, X, slice(s - 1, s + 7))]
        across = ref[(*pre, X - 1, slice(s, s + 8))] + ref[(*pre, X + 1, slice(s, s + 8))]
        return across + (low + ref[(*pre, X, slice(s + 1, s + 9))])

    def both(refs, pre, X, s):
        m, e = refs[0][(*pre, X, slice(s, s + 8))], refs[1][(*pre, X, slice(s, s + 8))]
        zm, ze = beside_z(m, e)
        return (m, beside_xy(refs[0], pre, X, s, m) + zm), (e, beside_xy(refs[1], pre, X, s, e) + ze)

    def one(src, dst, reach, moved, low, high, melt, u_tiles, tiles):
        warm = []
        for plane in (first, second):
            heat = (2.0 * (plane - moved).astype(f32) + 1.0) / planes.astype(f32) - 1.0
            warm.append([0.3 * heat - 0.15 * slope for slope in SLOPES])

        def potential(X, s):
            for half, (c, around) in enumerate(both(src, (3,), X, s)):
                p = [src[half][k, X, s : s + 8, :] for k in range(3)]
                value = (1.3 * c - 0.05 * around) + (0.3 * p[0] - 0.2 * p[1] + 0.1 * p[2])
                (u0, u1)[half][X, s : s + 8, :] = value

        def update(X, s):
            rows = slice(s, s + 8)
            flow = both((u0, u1), (), X, s)
            phases = [both(src, (k,), X, s) for k in range(3)]
            rates = [mo[k, X, rows, :] for k in range(3)]
            for half in range(2):
                c = src[half][3, X, rows, :]
                v, around = flow[half]
                new = [None, None, None, c + (0.05 * around - 0.3 * v)]
                sq = [w * w for w, _ in (p[half] for p in phases)]
                shared = 8.0 + 1.5 * ((sq[0] + sq[1]) + sq[2])
                for k in range(3):
                    w, near = phases[k][half]
                    grow = w + rates[k] * (near - w * (shared + w * (2.5 * w - 6.0)))
                    new[k] = grow - (w - sq[k]) * (warm[half][k] + 0.3 * SLOPES[k] * c)
                for k in range(4):
                    value = new[k]
                    if half == 0 and low is not None:
                        value = jnp.where(first >= low, value, 0.0)
                    if half == 1 and melt:
                        value = jnp.where(top, ex[k, X, rows, :], value)
                    if half == 1 and high is not None:
                        value = jnp.where(second < high, value, 0.0)
                    dst[half][k, X, rows, :] = value

        for X in range(7 - reach, 10 - reach):
            for s in u_tiles:
                potential(X, s)

        def row(X, carry, at=tiles):
            for ahead in u_tiles:
                potential(X + 2, ahead)
            for s in at:
                update(X, s)
            return carry

        if reach == 6:
            lax.fori_loop(2, 7, functools.partial(row, at=(4, 12, 20)), 0, unroll=5)
            lax.fori_loop(7, 17, row, 0, unroll=5)
            lax.fori_loop(17, 22, functools.partial(row, at=(4, 12, 20)), 0, unroll=5)
        else:
            lax.fori_loop(8 - reach, 16 + reach, row, 0, unroll=4)

    a, b = (a0, a1), (b0, b1)
    every = (0, 8, 16, 24)
    one(a, b, 6, 0, None, planes, False, every, every)
    one(b, a, 4, 0, s1, planes + s1, True, every, (4, 12, 20))
    one(a, b, 2, s1, s1, planes + s1, False, (5, 13, 21), (6, 14, 22))
    one(b, a, 0, s1, None, None, False, (7, 15, 23), (8, 16))

    total = s1 + s2
    for k in range(4):
        for x in range(8):
            for s in (0, 8):
                rows = slice(8 + s, 16 + s)
                melt = pltpu.roll(ex[k, 8 + x, rows, :], (s1 + 112) % 128, 1)
                above = jnp.where(top & (lane >= s1), melt, a1[k, 8 + x, rows, :])
                own = pltpu.roll(a0[k, 8 + x, rows, :], 128 - total, 1)
                above = pltpu.roll(above, 128 - total, 1)
                out[k, x, s : s + 8, :] = jnp.where(lane < 128 - total, own, above)


def kernel(fn, mib, out_shapes, scratch=(), scalars=0, hbm=False):
    def call(*args):
        specs = [pl.BlockSpec(memory_space=pltpu.HBM if hbm else pltpu.VMEM) for _ in args]
        specs[:scalars] = [pl.BlockSpec(memory_space=pltpu.SMEM)] * scalars
        return pl.pallas_call(
            fn,
            in_specs=specs,
            out_specs=[pl.BlockSpec(memory_space=pltpu.VMEM) for _ in out_shapes],
            out_shape=[jax.ShapeDtypeStruct(s, f32) for s in out_shapes],
            scratch_shapes=[pltpu.VMEM(s, f32) if isinstance(s, tuple) else s for s in scratch],
            compiler_params=pltpu.CompilerParams(vmem_limit_bytes=mib if mib > 1000 else mib << 20),
        )(*args)

    return call


def ring(value, axis, by):
    n = lax.axis_size(axis)
    return lax.ppermute(value, axis, [(i, (i + by) % n) for i in range(n)])


def from_above(value):
    n = lax.axis_size("gz")
    return lax.ppermute(value, "gz", [(i, i - 1) for i in range(1, n)])


def melt_above(melt):
    both = jnp.concatenate([melt[0], melt[1], jnp.zeros(melt.shape[1:4] + (ZE - 32,), f32)], axis=-1)
    phases = jnp.pad(jnp.concatenate([both[0], both[1], both[2]], axis=-1).reshape(128, 3 * ZE), ((0, 0), (0, 8)))
    c = jnp.pad(both[3], ((0, 1), (0, 0), (0, 0)))
    solute = jnp.pad(jnp.concatenate([c[0:3], c[3:6], c[6:9]], axis=-1).reshape(48, 3 * ZE), ((0, 0), (0, 8)))
    return jnp.concatenate([phases, solute], axis=0)


def body(fields, grain_ids, grain_angle, melt_planes, shifts):
    inputs = [pltpu.VMEM(grain_ids.shape, jnp.int32), melt_planes.shape[1:], pltpu.SemaphoreType.DMA((3,))]
    up, dn, own = kernel(pack_first, 4, [(Y_ROWS, 128)] * 2 + [fields.shape], inputs, hbm=True)(
        *(pltpu.with_memory_space_constraint(v, pltpu.HBM) for v in (fields, grain_ids, melt_planes))
    )
    ylo = ring(up, "gy", 1)
    yhi = ring(dn, "gy", -1)
    x1lo = ring(own, "gx", 1)
    x1hi = ring(own, "gx", -1)
    (low,) = kernel(pack_low, 2, [(Z_ROWS, 128)])(own)
    z1 = from_above(low)
    gz = lax.axis_index("gz").astype(jnp.int32)
    scal = jnp.stack([gz, shifts[0], shifts[1], jnp.int32(lax.axis_size("gz"))])
    mob, mown = kernel(own_columns, 2, [(8, 128), (3, 8, 16, 128)], scalars=1)(grain_angle, grain_ids)
    tiles = (4, 2, 8, 8, 128)
    yh, z2 = kernel(unpack_y, 2, [tiles, (8 * Z2_TILES, 128)])(ylo, yhi)
    z2 = from_above(z2)
    shapes = [(Z_ROWS, 128), tiles, (X2_ROWS, 128), (X2_ROWS, 128), (8, 128)]
    zp, eh, up2, dn2, moby = kernel(unpack_z, 4, shapes, [(416, 128)], scalars=2)(
        scal, grain_angle, z1, melt_above(melt_planes), mob, z2, ylo, yhi, yh
    )
    x2lo = ring(up2, "gx", 1)
    x2hi = ring(dn2, "gx", -1)
    block = (4, 26, 40, 128)
    (out,) = kernel(
        steps, 24, [(4, 8, 16, 128)], [block] * 4 + [block[1:]] * 2 + [(4, 24, 32, 128), (3, 24, 32, 128)], scalars=1
    )(scal, own, zp, mown, x1lo, x1hi, moby, yh, eh, x2lo, x2hi)
    return out


def solution(mesh):
    placed = (P(None, "gx", "gy", "gz"), P("gx", "gy"), P(), P(None, None, "gx", "gy", None), P())
    return jax.shard_map(
        body, mesh=mesh, in_specs=placed, out_specs=P(None, "gx", "gy", "gz"), check_vma=False
    )
```

```python
import functools

import jax
import jax.numpy as jnp
from jax import lax
from jax.experimental import pallas as pl
from jax.experimental.pallas import tpu as pltpu
from jax.sharding import PartitionSpec as P


f32 = jnp.float32
SLOPES = (0.5, 0.8, 1.1)
ZE = 40

Y_ROWS = 224
Y_MELT, Y_IDS = 208, 218
Z_ROWS = 176
Z2_TILES = 18
X2_ZP, X2_MOB = 272, 272 + Z_ROWS
X2_ROWS = X2_MOB + 16


def lanes(shape):
    return lax.broadcasted_iota(jnp.int32, shape, len(shape) - 1)


def subs(shape):
    return lax.broadcasted_iota(jnp.int32, shape, len(shape) - 2)


def three(a, b, c):
    lane = lanes(a.shape)
    out = jnp.where(lane < ZE, a, pltpu.roll(b, ZE, len(a.shape) - 1))
    return out if c is None else jnp.where(lane < 2 * ZE, out, pltpu.roll(c, 2 * ZE, len(a.shape) - 1))


def part(a, group):
    return a if group == 0 else pltpu.roll(a, 128 - ZE * group, len(a.shape) - 1)


def combined(c, p0, p1, p2):
    return c - 6.0 * p0 + 4.0 * p1 - 2.0 * p2


def even(axis):
    return lax.axis_index(axis) % 2 == 0


def swapped(flag, a, b):
    return jnp.where(flag, a, b), jnp.where(flag, b, a)


def pack_first(f_in, ids_in, melt_in, m1, m2, f, up, dn, ids, melt, sems):
    copies = [
        pltpu.make_async_copy(f_in, f, sems.at[0]),
        pltpu.make_async_copy(ids_in, ids, sems.at[1]),
        pltpu.make_async_copy(melt_in.at[0], melt, sems.at[2]),
    ]
    for copy in copies:
        copy.start()
    copies[0].wait()
    for x in range(8):
        up[8 * x : 8 * x + 8, :] = f[3, x, 8:16, :]
        up[8 * x : 8 * x + 1, :] = combined(f[3, x, 8:9, :], f[0, x, 9:10, :], f[1, x, 9:10, :], f[2, x, 9:10, :])
        dn[8 * x : 8 * x + 8, :] = f[3, x, 0:8, :]
        dn[8 * x + 7 : 8 * x + 8, :] = combined(f[3, x, 7:8, :], f[0, x, 6:7, :], f[1, x, 6:7, :], f[2, x, 6:7, :])
        for k in range(3):
            at = 64 + 18 * x + 6 * k
            up[at : at + 6, :] = f[k, x, 10:16, :]
            dn[at : at + 6, :] = f[k, x, 0:6, :]

    copies[1].wait()
    copies[2].wait()

    def beside(k, y):
        return jnp.concatenate([melt[k, x, y : y + 1, :] for x in range(8)], axis=1)

    m = Y_MELT
    up[m : m + 1, :] = combined(beside(3, 12), beside(0, 13), beside(1, 13), beside(2, 13))
    dn[m + 3 : m + 4, :] = combined(beside(3, 3), beside(0, 2), beside(1, 2), beside(2, 2))
    for j in range(3):
        up[m + 1 + j : m + 2 + j, :] = beside(3, 13 + j)
        dn[m + j : m + 1 + j, :] = beside(3, j)
    for k in range(3):
        for j in range(2):
            at = m + 4 + 2 * k + j
            up[at : at + 1, :] = beside(k, 14 + j)
            dn[at : at + 1, :] = beside(k, j)
    for out in (up, dn):
        out[Y_IDS : Y_IDS + 1, :] = jnp.concatenate([ids[x : x + 1, :].astype(f32) for x in range(8)], axis=1)
        out[Y_IDS + 1 : Y_ROWS, :] = jnp.zeros((Y_ROWS - Y_IDS - 1, 128), f32)
    m1[...], m2[...] = swapped(even("gy"), up[...], dn[...])


def pack_low(f, zp):
    for x in range(8):
        zp[16 * x : 16 * x + 16, :] = three(f[0, x], f[1, x], f[2, x])
    for x in range(3):
        zp[128 + 16 * x : 144 + 16 * x, :] = three(f[3, x], f[3, x + 3], f[3, x + 6] if x < 2 else None)


def mobility_of(grain, angles):
    angle = jnp.zeros(grain.shape, f32)
    for g in range(angles.shape[0]):
        angle = jnp.where(grain == float(g), angles[g], angle)
    return [1.0 + 0.6 * jnp.cos(4.0 * angle + 2.0944 * k) for k in range(3)]


def columns(mo, src, row, x, X, y, Y, n):
    hit = lanes((n, 128)) == 16 * x + y + subs((n, 128))
    for k in range(3):
        value = jnp.sum(jnp.where(hit, src[row + k : row + k + 1, :], 0.0), axis=1, keepdims=True)
        mo[k, X, Y : Y + n, :] = jnp.broadcast_to(0.05 * value, (n, 128))


def own_columns(angles, ids, mob, mown):
    grain = jnp.concatenate([ids[x : x + 1, :].astype(f32) for x in range(8)], axis=1)
    mob[...] = jnp.zeros(mob.shape, f32)
    for k, row in enumerate(mobility_of(grain, angles)):
        mob[k : k + 1, :] = row
    for x in range(8):
        columns(mown, mob, 0, x, x, 0, 0, 16)


def tiles_of(src, base, side, dst):
    for x in range(8):
        dst[3, side, x] = src[base + 8 * x : base + 8 * x + 8, :]
        for k in range(3):
            at = base + 64 + 18 * x + 6 * k
            dst[k, side, x] = jnp.zeros((8, 128), f32)
            dst[k, side, x, 2 - 2 * side : 8 - 2 * side, :] = src[at : at + 6, :]


def unpack_y(y1, y2, yh, z2, lo, hi):
    hi[...], lo[...] = swapped(even("gy"), y1[...], y2[...])
    tiles_of(lo, 0, 0, yh)
    tiles_of(hi, 0, 1, yh)

    def tile(t):
        return lo[8 * t : 8 * t + 8, :] if t < 26 else hi[8 * (t - 26) : 8 * (t - 26) + 8, :]

    for t in range(Z2_TILES):
        z2[8 * t : 8 * t + 8, :] = three(tile(t), tile(t + 18), tile(t + 36) if t + 36 < 52 else None)


def unpack_z(scal, angles, z1, meltp, mob, z2, lo, hi, yh, zp, eh, m1, m2, moby, flat, up, dn):
    top = scal[0] == scal[3] - 1
    zp[...] = jnp.where(top, meltp[...], z1[...])
    moby[...] = jnp.zeros(moby.shape, f32)
    for side, src in ((0, lo), (3, hi)):
        for k, row in enumerate(mobility_of(src[Y_IDS : Y_IDS + 1, :], angles)):
            moby[side + k : side + k + 1, :] = row

    for t in range(Z2_TILES):
        tile = z2[8 * t : 8 * t + 8, :]
        for g in range(3):
            if t + 18 * g < 52:
                flat[8 * (t + 18 * g) : 8 * (t + 18 * g) + 8, :] = part(tile, g)
    tiles_of(flat, 0, 0, eh)
    tiles_of(flat, 208, 1, eh)

    @pl.when(top)
    def _():
        eh[...] = jnp.zeros(eh.shape, f32)
        for side, src in ((0, lo), (1, hi)):
            for x in range(8):
                rows = src[Y_MELT : Y_MELT + 10, :]
                if x:
                    rows = pltpu.roll(src[Y_MELT : Y_MELT + 16, :], 128 - 16 * x, 1)
                eh[3, side, x, 4 - 4 * side : 8 - 4 * side, :] = rows[0:4]
                for k in range(3):
                    eh[k, side, x, 6 - 6 * side : 8 - 6 * side, :] = rows[4 + 2 * k : 6 + 2 * k]

    sub = subs((8, 128))
    for out, col in ((up, lambda dx: 8 - dx), (dn, lambda dx: dx - 1)):

        def corner(src, k, dx):
            if k == 3:
                return jnp.where(sub >= dx, src[3, 0, col(dx)], src[3, 1, col(8 - dx)])
            return jnp.where(sub > dx, src[k, 0, col(dx)], src[k, 1, col(7 - dx)])

        at = 0
        for dx in range(1, 8):
            out[at : at + 8, :] = corner(yh, 3, dx)
            at += 8
        for k in range(3):
            for dx in range(1, 7):
                out[at : at + 8, :] = corner(yh, k, dx)
                at += 8
        for i in range(3):
            out[at : at + 8, :] = three(corner(eh, 3, 1 + i), corner(eh, 3, 4 + i), corner(eh, 3, 7) if i == 0 else None)
            at += 8
        for dx in range(1, 7):
            out[at : at + 8, :] = three(corner(eh, 0, dx), corner(eh, 1, dx), corner(eh, 2, dx))
            at += 8
        out[X2_ZP:X2_MOB, :] = zp[...]
        out[X2_MOB : X2_MOB + 8, :] = moby[...]
        out[X2_MOB + 8 :, :] = mob[...]
    m1[...], m2[...] = swapped(even("gx"), up[...], dn[...])


def steps(scal, f, zp, mown, x1a, x1b, moby, yh, eh, x2a, x2b, out, a0, a1, b0, b1, u0, u1, ex, mo):
    gz, s1, s2, top = scal[0], scal[1], scal[2], scal[0] == scal[3] - 1
    planes = scal[3] * 128

    for k in range(4):
        a0[k, 8:16, 8:24, :] = f[k]
        for x in range(8):
            r = 16 * x if k < 3 else 128 + 16 * (x % 3)
            ex[k, 8 + x, 8:24, :] = part(zp[r : r + 16, :], k if k < 3 else x // 3)
        for side in range(2):
            a0[k, 8:16, 24 * side : 24 * side + 8, :] = yh[k, side]
            ex[k, 8:16, 24 * side : 24 * side + 8, :] = eh[k, side]
    mo[:, 8:16, 8:24, :] = mown[...]
    for x in range(8):
        columns(mo, moby, 0, x, 8 + x, 8, 0, 8)
        columns(mo, moby, 3, x, 8 + x, 0, 24, 8)

    def sides(x1lo, x1hi, x2lo, x2hi):
        for k in range(4):
            for x in range(8):
                a0[k, x, 8:24, :] = x1lo[k, x]
                a0[k, 16 + x, 8:24, :] = x1hi[k, x]
                r = X2_ZP + (16 * x if k < 3 else 128 + 16 * (x % 3))
                for src, X in ((x2lo, 0), (x2hi, 16)):
                    ex[k, X + x, 8:24, :] = part(src[r : r + 16, :], k if k < 3 else x // 3)
        for src, lo_col, hi_col in ((x2lo, lambda d: 8 - d, lambda d: 8 - d), (x2hi, lambda d: 15 + d, lambda d: 15 + d)):
            for k in (3, 0, 1, 2):
                for dx in range(1, 8 if k == 3 else 7):
                    at = 8 * (dx - 1) if k == 3 else 56 + 48 * k + 8 * (dx - 1)
                    tile = src[at : at + 8, :]
                    if k == 3:
                        above = part(src[200 + 8 * ((dx - 1) % 3) : 208 + 8 * ((dx - 1) % 3), :], (dx - 1) // 3)
                        other = 8 - dx
                    else:
                        above = part(src[224 + 8 * (dx - 1) : 232 + 8 * (dx - 1), :], k)
                        other = 7 - dx
                    a0[k, lo_col(dx), 0:8, :] = tile
                    a0[k, hi_col(other), 24:32, :] = tile
                    ex[k, lo_col(dx), 0:8, :] = above
                    ex[k, hi_col(other), 24:32, :] = above
        for x in range(8):
            for src, X in ((x2lo, x), (x2hi, 16 + x)):
                if 3 <= X < 21:
                    columns(mo, src, X2_MOB + 8, x, X, 0, 8, 16)
                    columns(mo, src, X2_MOB, x, X, 8, 0, 8)
                    columns(mo, src, X2_MOB + 3, x, X, 0, 24, 8)

    flag = even("gx")

    @pl.when(flag)
    def _():
        sides(x1b, x1a, x2b, x2a)

    @pl.when(jnp.logical_not(flag))
    def _():
        sides(x1a, x1b, x2a, x2b)

    lane = lanes((8, 128))
    first = gz * 128 + lane
    second = first + 128
    for k in range(4):
        for X in range(24):
            for s in range(0, 32, 8):
                a1[k, X, s : s + 8, :] = jnp.where(second < planes, ex[k, X, s : s + 8, :], 0.0)

    def beside_z(m, e):
        m1, e1, m9, e9 = pltpu.roll(m, 1, 1), pltpu.roll(e, 1, 1), pltpu.roll(m, 127, 1), pltpu.roll(e, 127, 1)
        return m1 + jnp.where(lane == 127, e9, m9), jnp.where(lane == 0, m1, e1) + e9

    def beside_xy(ref, pre, X, s, v):
        low = pltpu.roll(v, 1, 0) if s == 0 else ref[(*pre, X, slice(s - 1, s + 7))]
        across = ref[(*pre, X - 1, slice(s, s + 8))] + ref[(*pre, X + 1, slice(s, s + 8))]
        return across + (low + ref[(*pre, X, slice(s + 1, s + 9))])

    def both(refs, pre, X, s):
        m, e = refs[0][(*pre, X, slice(s, s + 8))], refs[1][(*pre, X, slice(s, s + 8))]
        zm, ze = beside_z(m, e)
        return (m, beside_xy(refs[0], pre, X, s, m) + zm), (e, beside_xy(refs[1], pre, X, s, e) + ze)

    def one(src, dst, reach, moved, low, high, melt, u_tiles, tiles):
        warm = []
        for plane in (first, second):
            heat = (2.0 * (plane - moved).astype(f32) + 1.0) / planes.astype(f32) - 1.0
            warm.append([0.3 * heat - 0.15 * slope for slope in SLOPES])

        def potential(X, s):
            for half, (c, around) in enumerate(both(src, (3,), X, s)):
                p = [src[half][k, X, s : s + 8, :] for k in range(3)]
                value = (1.3 * c - 0.05 * around) + (0.3 * p[0] - 0.2 * p[1] + 0.1 * p[2])
                (u0, u1)[half][X, s : s + 8, :] = value

        def update(X, s):
            rows = slice(s, s + 8)
            flow = both((u0, u1), (), X, s)
            phases = [both(src, (k,), X, s) for k in range(3)]
            rates = [mo[k, X, rows, :] for k in range(3)]
            for half in range(2):
                c = src[half][3, X, rows, :]
                v, around = flow[half]
                new = [None, None, None, c + (0.05 * around - 0.3 * v)]
                sq = [w * w for w, _ in (p[half] for p in phases)]
                shared = 8.0 + 1.5 * ((sq[0] + sq[1]) + sq[2])
                for k in range(3):
                    w, near = phases[k][half]
                    grow = w + rates[k] * (near - w * (shared + w * (2.5 * w - 6.0)))
                    new[k] = grow - (w - sq[k]) * (warm[half][k] + 0.3 * SLOPES[k] * c)
                for k in range(4):
                    value = new[k]
                    if half == 0 and low is not None:
                        value = jnp.where(first >= low, value, 0.0)
                    if half == 1 and melt:
                        value = jnp.where(top, ex[k, X, rows, :], value)
                    if half == 1 and high is not None:
                        value = jnp.where(second < high, value, 0.0)
                    dst[half][k, X, rows, :] = value

        for X in range(7 - reach, 10 - reach):
            for s in u_tiles:
                potential(X, s)

        def row(X, carry, at=tiles):
            for ahead in u_tiles:
                potential(X + 2, ahead)
            for s in at:
                update(X, s)
            return carry

        if reach == 6:
            lax.fori_loop(2, 7, functools.partial(row, at=(4, 12, 20)), 0, unroll=5)
            lax.fori_loop(7, 17, row, 0, unroll=5)
            lax.fori_loop(17, 22, functools.partial(row, at=(4, 12, 20)), 0, unroll=5)
        else:
            lax.fori_loop(8 - reach, 16 + reach, row, 0, unroll=4)

    a, b = (a0, a1), (b0, b1)
    every = (0, 8, 16, 24)
    one(a, b, 6, 0, None, planes, False, every, every)
    one(b, a, 4, 0, s1, planes + s1, True, every, (4, 12, 20))
    one(a, b, 2, s1, s1, planes + s1, False, (5, 13, 21), (6, 14, 22))
    one(b, a, 0, s1, None, None, False, (7, 15, 23), (8, 16))

    total = s1 + s2
    for k in range(4):
        for x in range(8):
            for s in (0, 8):
                rows = slice(8 + s, 16 + s)
                melt = pltpu.roll(ex[k, 8 + x, rows, :], (s1 + 112) % 128, 1)
                above = jnp.where(top & (lane >= s1), melt, a1[k, 8 + x, rows, :])
                own = pltpu.roll(a0[k, 8 + x, rows, :], 128 - total, 1)
                above = pltpu.roll(above, 128 - total, 1)
                out[k, x, s : s + 8, :] = jnp.where(lane < 128 - total, own, above)


def kernel(fn, mib, out_shapes, scratch=(), scalars=0, hbm=False):
    def call(*args):
        specs = [pl.BlockSpec(memory_space=pltpu.HBM if hbm else pltpu.VMEM) for _ in args]
        specs[:scalars] = [pl.BlockSpec(memory_space=pltpu.SMEM)] * scalars
        return pl.pallas_call(
            fn,
            in_specs=specs,
            out_specs=[pl.BlockSpec(memory_space=pltpu.VMEM) for _ in out_shapes],
            out_shape=[jax.ShapeDtypeStruct(s, f32) for s in out_shapes],
            scratch_shapes=[pltpu.VMEM(s, f32) if isinstance(s, tuple) else s for s in scratch],
            compiler_params=pltpu.CompilerParams(vmem_limit_bytes=mib if mib > 1000 else mib << 20),
        )(*args)

    return call


def swap(value, axis, stage):
    n = lax.axis_size(axis)
    return lax.ppermute(value, axis, [(i, (i + (1 if (i + stage) % 2 == 0 else -1)) % n) for i in range(n)])


def from_above(value):
    n = lax.axis_size("gz")
    return lax.ppermute(value, "gz", [(i, i - 1) for i in range(1, n)])


def melt_above(melt):
    both = jnp.concatenate([melt[0], melt[1], jnp.zeros(melt.shape[1:4] + (ZE - 32,), f32)], axis=-1)
    phases = jnp.pad(jnp.concatenate([both[0], both[1], both[2]], axis=-1).reshape(128, 3 * ZE), ((0, 0), (0, 8)))
    c = jnp.pad(both[3], ((0, 1), (0, 0), (0, 0)))
    solute = jnp.pad(jnp.concatenate([c[0:3], c[3:6], c[6:9]], axis=-1).reshape(48, 3 * ZE), ((0, 0), (0, 8)))
    return jnp.concatenate([phases, solute], axis=0)


def body(fields, grain_ids, grain_angle, melt_planes, shifts):
    inputs = [(Y_ROWS, 128), (Y_ROWS, 128), pltpu.VMEM(grain_ids.shape, jnp.int32), melt_planes.shape[1:], pltpu.SemaphoreType.DMA((3,))]
    m1, m2, own = kernel(pack_first, 4, [(Y_ROWS, 128)] * 2 + [fields.shape], inputs, hbm=True)(
        *(pltpu.with_memory_space_constraint(v, pltpu.HBM) for v in (fields, grain_ids, melt_planes))
    )
    y1 = swap(m1, "gy", 0)
    y2 = swap(m2, "gy", 1)
    x1a = swap(own, "gx", 0)
    x1b = swap(own, "gx", 1)
    (low,) = kernel(pack_low, 2, [(Z_ROWS, 128)])(own)
    z1 = from_above(low)
    gz = lax.axis_index("gz").astype(jnp.int32)
    scal = jnp.stack([gz, shifts[0], shifts[1], jnp.int32(lax.axis_size("gz"))])
    mob, mown = kernel(own_columns, 2, [(8, 128), (3, 8, 16, 128)], scalars=1)(grain_angle, grain_ids)
    tiles = (4, 2, 8, 8, 128)
    yh, z2, ylo, yhi = kernel(unpack_y, 2, [tiles, (8 * Z2_TILES, 128), (Y_ROWS, 128), (Y_ROWS, 128)])(y1, y2)
    z2 = from_above(z2)
    shapes = [(Z_ROWS, 128), tiles, (X2_ROWS, 128), (X2_ROWS, 128), (8, 128)]
    zp, eh, m1, m2, moby = kernel(unpack_z, 4, shapes, [(416, 128), (X2_ROWS, 128), (X2_ROWS, 128)], scalars=2)(
        scal, grain_angle, z1, melt_above(melt_planes), mob, z2, ylo, yhi, yh
    )
    x2a = swap(m1, "gx", 0)
    x2b = swap(m2, "gx", 1)
    block = (4, 26, 40, 128)
    (out,) = kernel(
        steps, 24, [(4, 8, 16, 128)], [block] * 4 + [block[1:]] * 2 + [(4, 24, 32, 128), (3, 24, 32, 128)], scalars=1
    )(scal, own, zp, mown, x1a, x1b, moby, yh, eh, x2a, x2b)
    return out


def solution(mesh):
    placed = (P(None, "gx", "gy", "gz"), P("gx", "gy"), P(), P(None, None, "gx", "gy", None), P())
    return jax.shard_map(
        body, mesh=mesh, in_specs=placed, out_specs=P(None, "gx", "gy", "gz"), check_vma=False
    )
```

```python
import functools

import jax
import jax.numpy as jnp
from jax import lax
from jax.experimental import pallas as pl
from jax.experimental.pallas import tpu as pltpu
from jax.sharding import PartitionSpec as P


f32 = jnp.float32
SLOPES = (0.5, 0.8, 1.1)
ZE = 40

Y_ROWS = 224
Y_MELT, Y_IDS = 208, 218
Z_ROWS = 176
Z2_TILES = 18
X2_ZP, X2_MOB = 272, 272 + Z_ROWS
X2_ROWS = X2_MOB + 16


def lanes(shape):
    return lax.broadcasted_iota(jnp.int32, shape, len(shape) - 1)


def subs(shape):
    return lax.broadcasted_iota(jnp.int32, shape, len(shape) - 2)


def three(a, b, c):
    lane = lanes(a.shape)
    out = jnp.where(lane < ZE, a, pltpu.roll(b, ZE, len(a.shape) - 1))
    return out if c is None else jnp.where(lane < 2 * ZE, out, pltpu.roll(c, 2 * ZE, len(a.shape) - 1))


def part(a, group):
    return a if group == 0 else pltpu.roll(a, 128 - ZE * group, len(a.shape) - 1)


def combined(c, p0, p1, p2):
    return c - 6.0 * p0 + 4.0 * p1 - 2.0 * p2


def even(axis):
    return lax.axis_index(axis) % 2 == 0


def swapped(flag, a, b):
    return jnp.where(flag, a, b), jnp.where(flag, b, a)


def pack_first(f_in, ids_in, melt_in, m1, m2, f, up, dn, ids, melt, sems):
    copies = [
        pltpu.make_async_copy(f_in, f, sems.at[0]),
        pltpu.make_async_copy(ids_in, ids, sems.at[1]),
        pltpu.make_async_copy(melt_in.at[0], melt, sems.at[2]),
    ]
    for copy in copies:
        copy.start()
    copies[0].wait()
    for x in range(8):
        up[8 * x : 8 * x + 8, :] = f[3, x, 8:16, :]
        up[8 * x : 8 * x + 1, :] = combined(f[3, x, 8:9, :], f[0, x, 9:10, :], f[1, x, 9:10, :], f[2, x, 9:10, :])
        dn[8 * x : 8 * x + 8, :] = f[3, x, 0:8, :]
        dn[8 * x + 7 : 8 * x + 8, :] = combined(f[3, x, 7:8, :], f[0, x, 6:7, :], f[1, x, 6:7, :], f[2, x, 6:7, :])
        for k in range(3):
            at = 64 + 18 * x + 6 * k
            up[at : at + 6, :] = f[k, x, 10:16, :]
            dn[at : at + 6, :] = f[k, x, 0:6, :]

    copies[1].wait()
    copies[2].wait()

    def beside(k, y):
        return jnp.concatenate([melt[k, x, y : y + 1, :] for x in range(8)], axis=1)

    m = Y_MELT
    up[m : m + 1, :] = combined(beside(3, 12), beside(0, 13), beside(1, 13), beside(2, 13))
    dn[m + 3 : m + 4, :] = combined(beside(3, 3), beside(0, 2), beside(1, 2), beside(2, 2))
    for j in range(3):
        up[m + 1 + j : m + 2 + j, :] = beside(3, 13 + j)
        dn[m + j : m + 1 + j, :] = beside(3, j)
    for k in range(3):
        for j in range(2):
            at = m + 4 + 2 * k + j
            up[at : at + 1, :] = beside(k, 14 + j)
            dn[at : at + 1, :] = beside(k, j)
    for out in (up, dn):
        out[Y_IDS : Y_IDS + 1, :] = jnp.concatenate([ids[x : x + 1, :].astype(f32) for x in range(8)], axis=1)
        out[Y_IDS + 1 : Y_ROWS, :] = jnp.zeros((Y_ROWS - Y_IDS - 1, 128), f32)
    m1[...], m2[...] = swapped(even("gy"), up[...], dn[...])


def pack_low(f, zp):
    for x in range(8):
        zp[16 * x : 16 * x + 16, :] = three(f[0, x], f[1, x], f[2, x])
    for x in range(3):
        zp[128 + 16 * x : 144 + 16 * x, :] = three(f[3, x], f[3, x + 3], f[3, x + 6] if x < 2 else None)


def mobility_of(grain, angles):
    angle = jnp.zeros(grain.shape, f32)
    for g in range(angles.shape[0] - 1):
        angle = jnp.where(grain == float(g), angles[g], angle)
    return [1.0 + 0.6 * jnp.cos(4.0 * angle + 2.0944 * k) for k in range(3)]


def columns(mo, src, row, x, X, y, Y, n):
    hit = lanes((n, 128)) == 16 * x + y + subs((n, 128))
    for k in range(3):
        value = jnp.sum(jnp.where(hit, src[row + k : row + k + 1, :], 0.0), axis=1, keepdims=True)
        mo[k, X, Y : Y + n, :] = jnp.broadcast_to(0.05 * value, (n, 128))


def block_columns(mob, moby, mown):
    for x in range(8):
        columns(mown, mob, 0, x, x, 0, 8, 16)
        columns(mown, moby, 0, x, x, 8, 0, 8)
        columns(mown, moby, 3, x, x, 0, 24, 8)


def tiles_of(src, base, side, dst):
    for x in range(8):
        dst[3, side, x] = src[base + 8 * x : base + 8 * x + 8, :]
        for k in range(3):
            at = base + 64 + 18 * x + 6 * k
            dst[k, side, x] = jnp.zeros((8, 128), f32)
            dst[k, side, x, 2 - 2 * side : 8 - 2 * side, :] = src[at : at + 6, :]


def unpack_y(y1, y2, yh, z2, lo, hi):
    hi[...], lo[...] = swapped(even("gy"), y1[...], y2[...])
    tiles_of(lo, 0, 0, yh)
    tiles_of(hi, 0, 1, yh)

    def tile(t):
        return lo[8 * t : 8 * t + 8, :] if t < 26 else hi[8 * (t - 26) : 8 * (t - 26) + 8, :]

    for t in range(Z2_TILES):
        z2[8 * t : 8 * t + 8, :] = three(tile(t), tile(t + 18), tile(t + 36) if t + 36 < 52 else None)


def unpack_z(angles, z1, meltp, mine, z2, lo, hi, yh, zp, eh, m1, m2, mob, moby, flat, up, dn):
    mob[...] = jnp.zeros(mob.shape, f32)
    for k, row in enumerate(mobility_of(mine[Y_IDS : Y_IDS + 1, :], angles)):
        mob[k : k + 1, :] = row
    top = angles[angles.shape[0] - 1] > 0.5
    zp[...] = jnp.where(top, meltp[...], z1[...])
    moby[...] = jnp.zeros(moby.shape, f32)
    for side, src in ((0, lo), (3, hi)):
        for k, row in enumerate(mobility_of(src[Y_IDS : Y_IDS + 1, :], angles)):
            moby[side + k : side + k + 1, :] = row

    for t in range(Z2_TILES):
        tile = z2[8 * t : 8 * t + 8, :]
        for g in range(3):
            if t + 18 * g < 52:
                flat[8 * (t + 18 * g) : 8 * (t + 18 * g) + 8, :] = part(tile, g)
    tiles_of(flat, 0, 0, eh)
    tiles_of(flat, 208, 1, eh)

    @pl.when(top)
    def _():
        eh[...] = jnp.zeros(eh.shape, f32)
        for side, src in ((0, lo), (1, hi)):
            for x in range(8):
                rows = src[Y_MELT : Y_MELT + 10, :]
                if x:
                    rows = pltpu.roll(src[Y_MELT : Y_MELT + 16, :], 128 - 16 * x, 1)
                eh[3, side, x, 4 - 4 * side : 8 - 4 * side, :] = rows[0:4]
                for k in range(3):
                    eh[k, side, x, 6 - 6 * side : 8 - 6 * side, :] = rows[4 + 2 * k : 6 + 2 * k]

    sub = subs((8, 128))
    for out, col in ((up, lambda dx: 8 - dx), (dn, lambda dx: dx - 1)):

        def corner(src, k, dx):
            if k == 3:
                return jnp.where(sub >= dx, src[3, 0, col(dx)], src[3, 1, col(8 - dx)])
            return jnp.where(sub > dx, src[k, 0, col(dx)], src[k, 1, col(7 - dx)])

        at = 0
        for dx in range(1, 8):
            out[at : at + 8, :] = corner(yh, 3, dx)
            at += 8
        for k in range(3):
            for dx in range(1, 7):
                out[at : at + 8, :] = corner(yh, k, dx)
                at += 8
        for i in range(3):
            out[at : at + 8, :] = three(corner(eh, 3, 1 + i), corner(eh, 3, 4 + i), corner(eh, 3, 7) if i == 0 else None)
            at += 8
        for dx in range(1, 7):
            out[at : at + 8, :] = three(corner(eh, 0, dx), corner(eh, 1, dx), corner(eh, 2, dx))
            at += 8
        out[X2_ZP:X2_MOB, :] = zp[...]
        out[X2_MOB : X2_MOB + 8, :] = moby[...]
        out[X2_MOB + 8 :, :] = mob[...]
    m1[...], m2[...] = swapped(even("gx"), up[...], dn[...])


def steps(scal, f, zp, mown, x1a, x1b, yh, eh, x2a, x2b, out, a0, a1, b0, b1, u0, u1, ex, mo):
    gz, s1, s2, top = scal[0], scal[1], scal[2], scal[0] == scal[3] - 1
    planes = scal[3] * 128

    for k in range(4):
        a0[k, 8:16, 8:24, :] = f[k]
        for x in range(8):
            r = 16 * x if k < 3 else 128 + 16 * (x % 3)
            ex[k, 8 + x, 8:24, :] = part(zp[r : r + 16, :], k if k < 3 else x // 3)
        for side in range(2):
            a0[k, 8:16, 24 * side : 24 * side + 8, :] = yh[k, side]
            ex[k, 8:16, 24 * side : 24 * side + 8, :] = eh[k, side]
    mo[:, 8:16, :, :] = mown[...]

    def sides(x1lo, x1hi, x2lo, x2hi):
        for k in range(4):
            for x in range(8):
                a0[k, x, 8:24, :] = x1lo[k, x]
                a0[k, 16 + x, 8:24, :] = x1hi[k, x]
                r = X2_ZP + (16 * x if k < 3 else 128 + 16 * (x % 3))
                for src, X in ((x2lo, 0), (x2hi, 16)):
                    ex[k, X + x, 8:24, :] = part(src[r : r + 16, :], k if k < 3 else x // 3)
        for src, lo_col, hi_col in ((x2lo, lambda d: 8 - d, lambda d: 8 - d), (x2hi, lambda d: 15 + d, lambda d: 15 + d)):
            for k in (3, 0, 1, 2):
                for dx in range(1, 8 if k == 3 else 7):
                    at = 8 * (dx - 1) if k == 3 else 56 + 48 * k + 8 * (dx - 1)
                    tile = src[at : at + 8, :]
                    if k == 3:
                        above = part(src[200 + 8 * ((dx - 1) % 3) : 208 + 8 * ((dx - 1) % 3), :], (dx - 1) // 3)
                        other = 8 - dx
                    else:
                        above = part(src[224 + 8 * (dx - 1) : 232 + 8 * (dx - 1), :], k)
                        other = 7 - dx
                    a0[k, lo_col(dx), 0:8, :] = tile
                    a0[k, hi_col(other), 24:32, :] = tile
                    ex[k, lo_col(dx), 0:8, :] = above
                    ex[k, hi_col(other), 24:32, :] = above
        for x in range(8):
            for src, X in ((x2lo, x), (x2hi, 16 + x)):
                if 3 <= X < 21:
                    columns(mo, src, X2_MOB + 8, x, X, 0, 8, 16)
                    columns(mo, src, X2_MOB, x, X, 8, 0, 8)
                    columns(mo, src, X2_MOB + 3, x, X, 0, 24, 8)

    flag = even("gx")

    @pl.when(flag)
    def _():
        sides(x1b, x1a, x2b, x2a)

    @pl.when(jnp.logical_not(flag))
    def _():
        sides(x1a, x1b, x2a, x2b)

    lane = lanes((8, 128))
    first = gz * 128 + lane
    second = first + 128
    for k in range(4):
        for X in range(24):
            for s in range(0, 32, 8):
                a1[k, X, s : s + 8, :] = jnp.where(second < planes, ex[k, X, s : s + 8, :], 0.0)

    def beside_z(m, e):
        m1, e1, m9, e9 = pltpu.roll(m, 1, 1), pltpu.roll(e, 1, 1), pltpu.roll(m, 127, 1), pltpu.roll(e, 127, 1)
        return m1 + jnp.where(lane == 127, e9, m9), jnp.where(lane == 0, m1, e1) + e9

    def beside_xy(ref, pre, X, s, v):
        low = pltpu.roll(v, 1, 0) if s == 0 else ref[(*pre, X, slice(s - 1, s + 7))]
        across = ref[(*pre, X - 1, slice(s, s + 8))] + ref[(*pre, X + 1, slice(s, s + 8))]
        return across + (low + ref[(*pre, X, slice(s + 1, s + 9))])

    def both(refs, pre, X, s):
        m, e = refs[0][(*pre, X, slice(s, s + 8))], refs[1][(*pre, X, slice(s, s + 8))]
        zm, ze = beside_z(m, e)
        return (m, beside_xy(refs[0], pre, X, s, m) + zm), (e, beside_xy(refs[1], pre, X, s, e) + ze)

    def one(src, dst, reach, moved, low, high, melt, u_tiles, tiles):
        warm = []
        for plane in (first, second):
            heat = (2.0 * (plane - moved).astype(f32) + 1.0) / planes.astype(f32) - 1.0
            warm.append([0.3 * heat - 0.15 * slope for slope in SLOPES])

        def potential(X, s):
            for half, (c, around) in enumerate(both(src, (3,), X, s)):
                p = [src[half][k, X, s : s + 8, :] for k in range(3)]
                value = (1.3 * c - 0.05 * around) + (0.3 * p[0] - 0.2 * p[1] + 0.1 * p[2])
                (u0, u1)[half][X, s : s + 8, :] = value

        def update(X, s):
            rows = slice(s, s + 8)
            flow = both((u0, u1), (), X, s)
            phases = [both(src, (k,), X, s) for k in range(3)]
            rates = [mo[k, X, rows, :] for k in range(3)]
            for half in range(2):
                c = src[half][3, X, rows, :]
                v, around = flow[half]
                new = [None, None, None, c + (0.05 * around - 0.3 * v)]
                sq = [w * w for w, _ in (p[half] for p in phases)]
                shared = 8.0 + 1.5 * ((sq[0] + sq[1]) + sq[2])
                for k in range(3):
                    w, near = phases[k][half]
                    grow = w + rates[k] * (near - w * (shared + w * (2.5 * w - 6.0)))
                    new[k] = grow - (w - sq[k]) * (warm[half][k] + 0.3 * SLOPES[k] * c)
                for k in range(4):
                    value = new[k]
                    if half == 0 and low is not None:
                        value = jnp.where(first >= low, value, 0.0)
                    if half == 1 and melt:
                        value = jnp.where(top, ex[k, X, rows, :], value)
                    if half == 1 and high is not None:
                        value = jnp.where(second < high, value, 0.0)
                    dst[half][k, X, rows, :] = value

        for X in range(7 - reach, 10 - reach):
            for s in u_tiles:
                potential(X, s)

        def row(X, carry, at=tiles):
            for ahead in u_tiles:
                potential(X + 2, ahead)
            for s in at:
                update(X, s)
            return carry

        if reach == 6:
            lax.fori_loop(2, 7, functools.partial(row, at=(4, 12, 20)), 0, unroll=5)
            lax.fori_loop(7, 17, row, 0, unroll=5)
            lax.fori_loop(17, 22, functools.partial(row, at=(4, 12, 20)), 0, unroll=5)
        else:
            lax.fori_loop(8 - reach, 16 + reach, row, 0, unroll=4)

    a, b = (a0, a1), (b0, b1)
    every = (0, 8, 16, 24)
    one(a, b, 6, 0, None, planes, False, every, every)
    one(b, a, 4, 0, s1, planes + s1, True, every, (4, 12, 20))
    one(a, b, 2, s1, s1, planes + s1, False, (5, 13, 21), (6, 14, 22))
    one(b, a, 0, s1, None, None, False, (7, 15, 23), (8, 16))

    total = s1 + s2
    for k in range(4):
        for x in range(8):
            for s in (0, 8):
                rows = slice(8 + s, 16 + s)
                melt = pltpu.roll(ex[k, 8 + x, rows, :], (s1 + 112) % 128, 1)
                above = jnp.where(top & (lane >= s1), melt, a1[k, 8 + x, rows, :])
                own = pltpu.roll(a0[k, 8 + x, rows, :], 128 - total, 1)
                above = pltpu.roll(above, 128 - total, 1)
                out[k, x, s : s + 8, :] = jnp.where(lane < 128 - total, own, above)


def kernel(fn, mib, out_shapes, scratch=(), scalars=0, hbm=False):
    def call(*args):
        specs = [pl.BlockSpec(memory_space=pltpu.HBM if hbm else pltpu.VMEM) for _ in args]
        specs[:scalars] = [pl.BlockSpec(memory_space=pltpu.SMEM)] * scalars
        return pl.pallas_call(
            fn,
            in_specs=specs,
            out_specs=[pl.BlockSpec(memory_space=pltpu.VMEM) for _ in out_shapes],
            out_shape=[jax.ShapeDtypeStruct(s, f32) for s in out_shapes],
            scratch_shapes=[pltpu.VMEM(s, f32) if isinstance(s, tuple) else s for s in scratch],
            compiler_params=pltpu.CompilerParams(vmem_limit_bytes=mib if mib > 1000 else mib << 20),
        )(*args)

    return call


def swap(value, axis, stage):
    n = lax.axis_size(axis)
    return lax.ppermute(value, axis, [(i, (i + (1 if (i + stage) % 2 == 0 else -1)) % n) for i in range(n)])


def from_above(value):
    n = lax.axis_size("gz")
    return lax.ppermute(value, "gz", [(i, i - 1) for i in range(1, n)])


def melt_above(melt):
    both = jnp.concatenate([melt[0], melt[1], jnp.zeros(melt.shape[1:4] + (ZE - 32,), f32)], axis=-1)
    phases = jnp.pad(jnp.concatenate([both[0], both[1], both[2]], axis=-1).reshape(128, 3 * ZE), ((0, 0), (0, 8)))
    c = jnp.pad(both[3], ((0, 1), (0, 0), (0, 0)))
    solute = jnp.pad(jnp.concatenate([c[0:3], c[3:6], c[6:9]], axis=-1).reshape(48, 3 * ZE), ((0, 0), (0, 8)))
    return jnp.concatenate([phases, solute], axis=0)


def body(fields, grain_ids, grain_angle, melt_planes, shifts):
    inputs = [(Y_ROWS, 128), (Y_ROWS, 128), pltpu.VMEM(grain_ids.shape, jnp.int32), melt_planes.shape[1:], pltpu.SemaphoreType.DMA((3,))]
    m1, m2, own = kernel(pack_first, 4, [(Y_ROWS, 128)] * 2 + [fields.shape], inputs, hbm=True)(
        *(pltpu.with_memory_space_constraint(v, pltpu.HBM) for v in (fields, grain_ids, melt_planes))
    )
    y1 = swap(m1, "gy", 0)
    y2 = swap(m2, "gy", 1)
    x1a = swap(own, "gx", 0)
    x1b = swap(own, "gx", 1)
    (low,) = kernel(pack_low, 2, [(Z_ROWS, 128)])(own)
    z1 = from_above(low)
    gz = lax.axis_index("gz").astype(jnp.int32)
    grains = grain_angle.shape[0]
    at_top = (gz == lax.axis_size("gz") - 1).astype(f32)
    angles = jnp.pad(grain_angle, (0, 1)) + jnp.where(jnp.arange(grains + 1) == grains, at_top, 0.0)
    scal = jnp.stack([gz, shifts[0], shifts[1], jnp.int32(lax.axis_size("gz"))])
    tiles = (4, 2, 8, 8, 128)
    yh, z2, ylo, yhi = kernel(unpack_y, 2, [tiles, (8 * Z2_TILES, 128), (Y_ROWS, 128), (Y_ROWS, 128)])(y1, y2)
    z2 = from_above(z2)
    shapes = [(Z_ROWS, 128), tiles, (X2_ROWS, 128), (X2_ROWS, 128), (8, 128), (8, 128)]
    zp, eh, x2m1, x2m2, mob, moby = kernel(unpack_z, 4, shapes, [(416, 128), (X2_ROWS, 128), (X2_ROWS, 128)], scalars=1)(
        angles, z1, melt_above(melt_planes), m1, z2, ylo, yhi, yh
    )
    x2a = swap(x2m1, "gx", 0)
    x2b = swap(x2m2, "gx", 1)
    (mown,) = kernel(block_columns, 2, [(3, 8, 32, 128)])(mob, moby)
    block = (4, 26, 40, 128)
    (out,) = kernel(
        steps, 24, [(4, 8, 16, 128)], [block] * 4 + [block[1:]] * 2 + [(4, 24, 32, 128), (3, 24, 32, 128)], scalars=1
    )(scal, own, zp, mown, x1a, x1b, yh, eh, x2a, x2b)
    return out


def solution(mesh):
    placed = (P(None, "gx", "gy", "gz"), P("gx", "gy"), P(), P(None, None, "gx", "gy", None), P())
    return jax.shard_map(
        body, mesh=mesh, in_specs=placed, out_specs=P(None, "gx", "gy", "gz"), check_vma=False
    )
```

```python
import functools

import jax
import jax.numpy as jnp
from jax import lax
from jax.experimental import pallas as pl
from jax.experimental.pallas import tpu as pltpu
from jax.sharding import PartitionSpec as P


f32 = jnp.float32
SLOPES = (0.5, 0.8, 1.1)
ZE = 40

Y_ROWS = 224
Y_MELT, Y_IDS = 208, 218
Z_ROWS = 176
Z2_TILES = 18
X2_ZP, X2_MOB = 272, 272 + Z_ROWS
X2_ROWS = X2_MOB + 16


def lanes(shape):
    return lax.broadcasted_iota(jnp.int32, shape, len(shape) - 1)


def subs(shape):
    return lax.broadcasted_iota(jnp.int32, shape, len(shape) - 2)


def three(a, b, c):
    lane = lanes(a.shape)
    out = jnp.where(lane < ZE, a, pltpu.roll(b, ZE, len(a.shape) - 1))
    return out if c is None else jnp.where(lane < 2 * ZE, out, pltpu.roll(c, 2 * ZE, len(a.shape) - 1))


def part(a, group):
    return a if group == 0 else pltpu.roll(a, 128 - ZE * group, len(a.shape) - 1)


def combined(c, p0, p1, p2):
    return c - 6.0 * p0 + 4.0 * p1 - 2.0 * p2


def even(axis):
    return lax.axis_index(axis) % 2 == 0


def swapped(flag, a, b):
    return jnp.where(flag, a, b), jnp.where(flag, b, a)


def pack_first(f_in, ids_in, melt_in, m1, m2, f, up, dn, ids, melt, sems):
    copies = [
        pltpu.make_async_copy(f_in, f, sems.at[0]),
        pltpu.make_async_copy(ids_in, ids, sems.at[1]),
        pltpu.make_async_copy(melt_in.at[0], melt, sems.at[2]),
    ]
    for copy in copies:
        copy.start()
    copies[0].wait()
    for x in range(8):
        up[8 * x : 8 * x + 8, :] = f[3, x, 8:16, :]
        up[8 * x : 8 * x + 1, :] = combined(f[3, x, 8:9, :], f[0, x, 9:10, :], f[1, x, 9:10, :], f[2, x, 9:10, :])
        dn[8 * x : 8 * x + 8, :] = f[3, x, 0:8, :]
        dn[8 * x + 7 : 8 * x + 8, :] = combined(f[3, x, 7:8, :], f[0, x, 6:7, :], f[1, x, 6:7, :], f[2, x, 6:7, :])
        for k in range(3):
            at = 64 + 18 * x + 6 * k
            up[at : at + 6, :] = f[k, x, 10:16, :]
            dn[at : at + 6, :] = f[k, x, 0:6, :]

    copies[1].wait()
    copies[2].wait()

    def beside(k, y):
        return jnp.concatenate([melt[k, x, y : y + 1, :] for x in range(8)], axis=1)

    m = Y_MELT
    up[m : m + 1, :] = combined(beside(3, 12), beside(0, 13), beside(1, 13), beside(2, 13))
    dn[m + 3 : m + 4, :] = combined(beside(3, 3), beside(0, 2), beside(1, 2), beside(2, 2))
    for j in range(3):
        up[m + 1 + j : m + 2 + j, :] = beside(3, 13 + j)
        dn[m + j : m + 1 + j, :] = beside(3, j)
    for k in range(3):
        for j in range(2):
            at = m + 4 + 2 * k + j
            up[at : at + 1, :] = beside(k, 14 + j)
            dn[at : at + 1, :] = beside(k, j)
    for out in (up, dn):
        out[Y_IDS : Y_IDS + 1, :] = jnp.concatenate([ids[x : x + 1, :].astype(f32) for x in range(8)], axis=1)
        out[Y_IDS + 1 : Y_ROWS, :] = jnp.zeros((Y_ROWS - Y_IDS - 1, 128), f32)
    m1[...], m2[...] = swapped(even("gy"), dn[...], up[...])


def pack_low(f, zp):
    for x in range(8):
        zp[16 * x : 16 * x + 16, :] = three(f[0, x], f[1, x], f[2, x])
    for x in range(3):
        zp[128 + 16 * x : 144 + 16 * x, :] = three(f[3, x], f[3, x + 3], f[3, x + 6] if x < 2 else None)


def mobility_of(grain, angles):
    angle = jnp.zeros(grain.shape, f32)
    for g in range(angles.shape[0] - 1):
        angle = jnp.where(grain == float(g), angles[g], angle)
    return [1.0 + 0.6 * jnp.cos(4.0 * angle + 2.0944 * k) for k in range(3)]


def columns(mo, src, row, x, X, y, Y, n):
    hit = lanes((n, 128)) == 16 * x + y + subs((n, 128))
    for k in range(3):
        value = jnp.sum(jnp.where(hit, src[row + k : row + k + 1, :], 0.0), axis=1, keepdims=True)
        mo[k, X, Y : Y + n, :] = jnp.broadcast_to(0.05 * value, (n, 128))


def block_columns(mob, moby, mown):
    for x in range(8):
        columns(mown, mob, 0, x, x, 0, 8, 16)
        columns(mown, moby, 0, x, x, 8, 0, 8)
        columns(mown, moby, 3, x, x, 0, 24, 8)


def tiles_of(src, base, side, dst):
    for x in range(8):
        dst[3, side, x] = src[base + 8 * x : base + 8 * x + 8, :]
        for k in range(3):
            at = base + 64 + 18 * x + 6 * k
            dst[k, side, x] = jnp.zeros((8, 128), f32)
            dst[k, side, x, 2 - 2 * side : 8 - 2 * side, :] = src[at : at + 6, :]


def unpack_y(y1, y2, yh, z2, lo, hi):
    lo[...], hi[...] = swapped(even("gy"), y1[...], y2[...])
    tiles_of(lo, 0, 0, yh)
    tiles_of(hi, 0, 1, yh)

    def tile(t):
        return lo[8 * t : 8 * t + 8, :] if t < 26 else hi[8 * (t - 26) : 8 * (t - 26) + 8, :]

    for t in range(Z2_TILES):
        z2[8 * t : 8 * t + 8, :] = three(tile(t), tile(t + 18), tile(t + 36) if t + 36 < 52 else None)


def unpack_z(angles, z1, meltp, mine, z2, lo, hi, yh, zp, eh, m1, m2, mob, moby, flat, up, dn):
    mob[...] = jnp.zeros(mob.shape, f32)
    for k, row in enumerate(mobility_of(mine[Y_IDS : Y_IDS + 1, :], angles)):
        mob[k : k + 1, :] = row
    top = angles[angles.shape[0] - 1] > 0.5
    zp[...] = jnp.where(top, meltp[...], z1[...])
    moby[...] = jnp.zeros(moby.shape, f32)
    for side, src in ((0, lo), (3, hi)):
        for k, row in enumerate(mobility_of(src[Y_IDS : Y_IDS + 1, :], angles)):
            moby[side + k : side + k + 1, :] = row

    for t in range(Z2_TILES):
        tile = z2[8 * t : 8 * t + 8, :]
        for g in range(3):
            if t + 18 * g < 52:
                flat[8 * (t + 18 * g) : 8 * (t + 18 * g) + 8, :] = part(tile, g)
    tiles_of(flat, 0, 0, eh)
    tiles_of(flat, 208, 1, eh)

    @pl.when(top)
    def _():
        eh[...] = jnp.zeros(eh.shape, f32)
        for side, src in ((0, lo), (1, hi)):
            for x in range(8):
                rows = src[Y_MELT : Y_MELT + 10, :]
                if x:
                    rows = pltpu.roll(src[Y_MELT : Y_MELT + 16, :], 128 - 16 * x, 1)
                eh[3, side, x, 4 - 4 * side : 8 - 4 * side, :] = rows[0:4]
                for k in range(3):
                    eh[k, side, x, 6 - 6 * side : 8 - 6 * side, :] = rows[4 + 2 * k : 6 + 2 * k]

    sub = subs((8, 128))
    for out, col in ((up, lambda dx: 8 - dx), (dn, lambda dx: dx - 1)):

        def corner(src, k, dx):
            if k == 3:
                return jnp.where(sub >= dx, src[3, 0, col(dx)], src[3, 1, col(8 - dx)])
            return jnp.where(sub > dx, src[k, 0, col(dx)], src[k, 1, col(7 - dx)])

        at = 0
        for dx in range(1, 8):
            out[at : at + 8, :] = corner(yh, 3, dx)
            at += 8
        for k in range(3):
            for dx in range(1, 7):
                out[at : at + 8, :] = corner(yh, k, dx)
                at += 8
        for i in range(3):
            out[at : at + 8, :] = three(corner(eh, 3, 1 + i), corner(eh, 3, 4 + i), corner(eh, 3, 7) if i == 0 else None)
            at += 8
        for dx in range(1, 7):
            out[at : at + 8, :] = three(corner(eh, 0, dx), corner(eh, 1, dx), corner(eh, 2, dx))
            at += 8
        out[X2_ZP:X2_MOB, :] = zp[...]
        out[X2_MOB : X2_MOB + 8, :] = moby[...]
        out[X2_MOB + 8 :, :] = mob[...]
    m1[...], m2[...] = swapped(even("gx"), up[...], dn[...])


def steps(scal, f, zp, mown, x1a, x1b, yh, eh, x2a, x2b, out, a0, a1, b0, b1, u0, u1, ex, mo):
    gz, s1, s2, top = scal[0], scal[1], scal[2], scal[0] == scal[3] - 1
    planes = scal[3] * 128

    for k in range(4):
        a0[k, 8:16, 8:24, :] = f[k]
        for x in range(8):
            r = 16 * x if k < 3 else 128 + 16 * (x % 3)
            ex[k, 8 + x, 8:24, :] = part(zp[r : r + 16, :], k if k < 3 else x // 3)
        for side in range(2):
            a0[k, 8:16, 24 * side : 24 * side + 8, :] = yh[k, side]
            ex[k, 8:16, 24 * side : 24 * side + 8, :] = eh[k, side]
    mo[:, 8:16, :, :] = mown[...]

    def sides(x1lo, x1hi, x2lo, x2hi):
        for k in range(4):
            for x in range(8):
                a0[k, x, 8:24, :] = x1lo[k, x]
                a0[k, 16 + x, 8:24, :] = x1hi[k, x]
                r = X2_ZP + (16 * x if k < 3 else 128 + 16 * (x % 3))
                for src, X in ((x2lo, 0), (x2hi, 16)):
                    ex[k, X + x, 8:24, :] = part(src[r : r + 16, :], k if k < 3 else x // 3)
        for src, lo_col, hi_col in ((x2lo, lambda d: 8 - d, lambda d: 8 - d), (x2hi, lambda d: 15 + d, lambda d: 15 + d)):
            for k in (3, 0, 1, 2):
                for dx in range(1, 8 if k == 3 else 7):
                    at = 8 * (dx - 1) if k == 3 else 56 + 48 * k + 8 * (dx - 1)
                    tile = src[at : at + 8, :]
                    if k == 3:
                        above = part(src[200 + 8 * ((dx - 1) % 3) : 208 + 8 * ((dx - 1) % 3), :], (dx - 1) // 3)
                        other = 8 - dx
                    else:
                        above = part(src[224 + 8 * (dx - 1) : 232 + 8 * (dx - 1), :], k)
                        other = 7 - dx
                    a0[k, lo_col(dx), 0:8, :] = tile
                    a0[k, hi_col(other), 24:32, :] = tile
                    ex[k, lo_col(dx), 0:8, :] = above
                    ex[k, hi_col(other), 24:32, :] = above
        for x in range(8):
            for src, X in ((x2lo, x), (x2hi, 16 + x)):
                if 3 <= X < 21:
                    columns(mo, src, X2_MOB + 8, x, X, 0, 8, 16)
                    columns(mo, src, X2_MOB, x, X, 8, 0, 8)
                    columns(mo, src, X2_MOB + 3, x, X, 0, 24, 8)

    flag = even("gx")

    @pl.when(flag)
    def _():
        sides(x1b, x1a, x2b, x2a)

    @pl.when(jnp.logical_not(flag))
    def _():
        sides(x1a, x1b, x2a, x2b)

    lane = lanes((8, 128))
    first = gz * 128 + lane
    second = first + 128
    for k in range(4):
        for X in range(24):
            for s in range(0, 32, 8):
                a1[k, X, s : s + 8, :] = jnp.where(second < planes, ex[k, X, s : s + 8, :], 0.0)

    def beside_z(m, e):
        m1, e1, m9, e9 = pltpu.roll(m, 1, 1), pltpu.roll(e, 1, 1), pltpu.roll(m, 127, 1), pltpu.roll(e, 127, 1)
        return m1 + jnp.where(lane == 127, e9, m9), jnp.where(lane == 0, m1, e1) + e9

    def beside_xy(ref, pre, X, s, v):
        low = pltpu.roll(v, 1, 0) if s == 0 else ref[(*pre, X, slice(s - 1, s + 7))]
        across = ref[(*pre, X - 1, slice(s, s + 8))] + ref[(*pre, X + 1, slice(s, s + 8))]
        return across + (low + ref[(*pre, X, slice(s + 1, s + 9))])

    def both(refs, pre, X, s):
        m, e = refs[0][(*pre, X, slice(s, s + 8))], refs[1][(*pre, X, slice(s, s + 8))]
        zm, ze = beside_z(m, e)
        return (m, beside_xy(refs[0], pre, X, s, m) + zm), (e, beside_xy(refs[1], pre, X, s, e) + ze)

    def one(src, dst, reach, moved, low, high, melt, u_tiles, tiles):
        warm = []
        for plane in (first, second):
            heat = (2.0 * (plane - moved).astype(f32) + 1.0) / planes.astype(f32) - 1.0
            warm.append([0.3 * heat - 0.15 * slope for slope in SLOPES])

        def potential(X, s):
            for half, (c, around) in enumerate(both(src, (3,), X, s)):
                p = [src[half][k, X, s : s + 8, :] for k in range(3)]
                value = (1.3 * c - 0.05 * around) + (0.3 * p[0] - 0.2 * p[1] + 0.1 * p[2])
                (u0, u1)[half][X, s : s + 8, :] = value

        def update(X, s):
            rows = slice(s, s + 8)
            flow = both((u0, u1), (), X, s)
            phases = [both(src, (k,), X, s) for k in range(3)]
            rates = [mo[k, X, rows, :] for k in range(3)]
            for half in range(2):
                c = src[half][3, X, rows, :]
                v, around = flow[half]
                new = [None, None, None, c + (0.05 * around - 0.3 * v)]
                sq = [w * w for w, _ in (p[half] for p in phases)]
                shared = 8.0 + 1.5 * ((sq[0] + sq[1]) + sq[2])
                for k in range(3):
                    w, near = phases[k][half]
                    grow = w + rates[k] * (near - w * (shared + w * (2.5 * w - 6.0)))
                    new[k] = grow - (w - sq[k]) * (warm[half][k] + 0.3 * SLOPES[k] * c)
                for k in range(4):
                    value = new[k]
                    if half == 0 and low is not None:
                        value = jnp.where(first >= low, value, 0.0)
                    if half == 1 and melt:
                        value = jnp.where(top, ex[k, X, rows, :], value)
                    if half == 1 and high is not None:
                        value = jnp.where(second < high, value, 0.0)
                    dst[half][k, X, rows, :] = value

        for X in range(7 - reach, 10 - reach):
            for s in u_tiles:
                potential(X, s)

        def row(X, carry, at=tiles):
            for ahead in u_tiles:
                potential(X + 2, ahead)
            for s in at:
                update(X, s)
            return carry

        if reach == 6:
            lax.fori_loop(2, 7, functools.partial(row, at=(4, 12, 20)), 0, unroll=5)
            lax.fori_loop(7, 17, row, 0, unroll=5)
            lax.fori_loop(17, 22, functools.partial(row, at=(4, 12, 20)), 0, unroll=5)
        else:
            lax.fori_loop(8 - reach, 16 + reach, row, 0, unroll=4)

    a, b = (a0, a1), (b0, b1)
    every = (0, 8, 16, 24)
    one(a, b, 6, 0, None, planes, False, every, every)
    one(b, a, 4, 0, s1, planes + s1, True, every, (4, 12, 20))
    one(a, b, 2, s1, s1, planes + s1, False, (5, 13, 21), (6, 14, 22))
    one(b, a, 0, s1, None, None, False, (7, 15, 23), (8, 16))

    total = s1 + s2
    for k in range(4):
        for x in range(8):
            for s in (0, 8):
                rows = slice(8 + s, 16 + s)
                melt = pltpu.roll(ex[k, 8 + x, rows, :], (s1 + 112) % 128, 1)
                above = jnp.where(top & (lane >= s1), melt, a1[k, 8 + x, rows, :])
                own = pltpu.roll(a0[k, 8 + x, rows, :], 128 - total, 1)
                above = pltpu.roll(above, 128 - total, 1)
                out[k, x, s : s + 8, :] = jnp.where(lane < 128 - total, own, above)


def kernel(fn, mib, out_shapes, scratch=(), scalars=0, hbm=False):
    def call(*args):
        specs = [pl.BlockSpec(memory_space=pltpu.HBM if hbm else pltpu.VMEM) for _ in args]
        specs[:scalars] = [pl.BlockSpec(memory_space=pltpu.SMEM)] * scalars
        return pl.pallas_call(
            fn,
            in_specs=specs,
            out_specs=[pl.BlockSpec(memory_space=pltpu.VMEM) for _ in out_shapes],
            out_shape=[jax.ShapeDtypeStruct(s, f32) for s in out_shapes],
            scratch_shapes=[pltpu.VMEM(s, f32) if isinstance(s, tuple) else s for s in scratch],
            compiler_params=pltpu.CompilerParams(vmem_limit_bytes=mib if mib > 1000 else mib << 20),
        )(*args)

    return call


def swap(value, axis, stage):
    n = lax.axis_size(axis)
    return lax.ppermute(value, axis, [(i, (i + (1 if (i + stage) % 2 == 0 else -1)) % n) for i in range(n)])


def from_above(value):
    n = lax.axis_size("gz")
    return lax.ppermute(value, "gz", [(i, i - 1) for i in range(1, n)])


def melt_above(melt):
    both = jnp.concatenate([melt[0], melt[1], jnp.zeros(melt.shape[1:4] + (ZE - 32,), f32)], axis=-1)
    phases = jnp.pad(jnp.concatenate([both[0], both[1], both[2]], axis=-1).reshape(128, 3 * ZE), ((0, 0), (0, 8)))
    c = jnp.pad(both[3], ((0, 1), (0, 0), (0, 0)))
    solute = jnp.pad(jnp.concatenate([c[0:3], c[3:6], c[6:9]], axis=-1).reshape(48, 3 * ZE), ((0, 0), (0, 8)))
    return jnp.concatenate([phases, solute], axis=0)


def body(fields, grain_ids, grain_angle, melt_planes, shifts):
    inputs = [(Y_ROWS, 128), (Y_ROWS, 128), pltpu.VMEM(grain_ids.shape, jnp.int32), melt_planes.shape[1:], pltpu.SemaphoreType.DMA((3,))]
    m1, m2, own = kernel(pack_first, 4, [(Y_ROWS, 128)] * 2 + [fields.shape], inputs, hbm=True)(
        *(pltpu.with_memory_space_constraint(v, pltpu.HBM) for v in (fields, grain_ids, melt_planes))
    )
    y1 = swap(m1, "gy", 1)
    y2 = swap(m2, "gy", 0)
    x1a = swap(own, "gx", 0)
    x1b = swap(own, "gx", 1)
    (low,) = kernel(pack_low, 2, [(Z_ROWS, 128)])(own)
    z1 = from_above(low)
    gz = lax.axis_index("gz").astype(jnp.int32)
    grains = grain_angle.shape[0]
    at_top = (gz == lax.axis_size("gz") - 1).astype(f32)
    angles = jnp.pad(grain_angle, (0, 1)) + jnp.where(jnp.arange(grains + 1) == grains, at_top, 0.0)
    scal = jnp.stack([gz, shifts[0], shifts[1], jnp.int32(lax.axis_size("gz"))])
    tiles = (4, 2, 8, 8, 128)
    yh, z2, ylo, yhi = kernel(unpack_y, 2, [tiles, (8 * Z2_TILES, 128), (Y_ROWS, 128), (Y_ROWS, 128)])(y1, y2)
    z2 = from_above(z2)
    shapes = [(Z_ROWS, 128), tiles, (X2_ROWS, 128), (X2_ROWS, 128), (8, 128), (8, 128)]
    zp, eh, x2m1, x2m2, mob, moby = kernel(unpack_z, 4, shapes, [(416, 128), (X2_ROWS, 128), (X2_ROWS, 128)], scalars=1)(
        angles, z1, melt_above(melt_planes), m1, z2, ylo, yhi, yh
    )
    x2a = swap(x2m1, "gx", 0)
    x2b = swap(x2m2, "gx", 1)
    (mown,) = kernel(block_columns, 2, [(3, 8, 32, 128)])(mob, moby)
    block = (4, 26, 40, 128)
    (out,) = kernel(
        steps, 24, [(4, 8, 16, 128)], [block] * 4 + [block[1:]] * 2 + [(4, 24, 32, 128), (3, 24, 32, 128)], scalars=1
    )(scal, own, zp, mown, x1a, x1b, yh, eh, x2a, x2b)
    return out


def solution(mesh):
    placed = (P(None, "gx", "gy", "gz"), P("gx", "gy"), P(), P(None, None, "gx", "gy", None), P())
    return jax.shard_map(
        body, mesh=mesh, in_specs=placed, out_specs=P(None, "gx", "gy", "gz"), check_vma=False
    )
```
